128 devices in a mesh: band: 32 (over x, z, core), lev: 4 (over y).
Axes of the slice: x: 4, y: 4, z: 4, core: 2. Of those that a mesh axis runs over, the one named last changes fastest.
Arguments:
- checkpoints: float32 [4, 4, 32, 2, 256, 256], P(None, None, 'lev', None, 'band'), may hold values from -0.4 to 0.4
- final_cot: float32 [4, 32, 2, 256, 256], P(None, 'lev', None, 'band'), may hold values from -6 to 6
- obs_cot: float32 [4, 4, 32, 256, 512], P(None, None, None, 'band', 'lev'), may hold values from -0.2 to 0.2
- obs_time: int32 [4], replicated, may hold values from 0 to 3
- wave_order: int32 [256], replicated, may hold values from 0 to 255, each once
- legendre: bfloat16 [256, 256, 256], P('band'), may hold values from -0.375 to 0.375
- w_in: bfloat16 [128, 512], replicated, may hold values from -0.5 to 0.5
- w_out: bfloat16 [512, 128], replicated, may hold values from -0.25 to 0.25
- bias: float32 [512], replicated, may hold values from -3 to 3
Outputs:
- grad_state: float32 [4, 32, 2, 256, 256], P(None, 'lev', None, 'band')
- grad_w_in: float32 [128, 512], replicated
- grad_w_out: float32 [512, 128], replicated
- grad_bias: float32 [512], replicated
The draws below stay inside these ranges and needn't reach their ends.
Inputs may be any that keep to these rules, and one draw needn't show every extreme that they name: `obs_time`: each number names a step of the rollout. `wave_order`: each of the 256 zonal wavenumbers once.
All inputs are finite; a program needn't handle non-finite values.
Results may differ from the reference program's by a relative error of at most 0.014.
Values may be sent and summed in bfloat16 or wider, within the bound.
No kernel may reach another device: no remote copies, remote signals or barrier semaphores. Data moves between devices by JAX's collectives and lax.ppermute only.
A program may use at most 128 MiB of HBM per device.

```python
import jax
import jax.numpy as jnp
from jax import lax

M = 256
LAT = 256
LON = 512
LEV = 32
VARS = 4
HID = 512
STEPS = 4
NOBS = 4


def plant(result, stream_key, least, largest):
    longest = result.shape.index(max(result.shape))
    spots = []
    for shift in (0, 1):
        where = [jax.random.randint(jax.random.fold_in(stream_key, axis), (), 0, length) for axis, length in enumerate(result.shape)]
        where[longest] = (where[longest] + shift) % result.shape[longest]
        spots.append(tuple(where))
    return result.at[spots[0]].set(least).at[spots[1]].set(largest)


def steps_of(rng, shape, shards, smallest, top_value):
    level = 1.0
    for position, parts in shards:
        steps = jax.random.uniform(jax.random.fold_in(jax.random.fold_in(rng, 6), position), (parts,), jnp.float32, smallest / len(shards), top_value / len(shards))
        level = level * jnp.repeat(jnp.exp(steps), shape[position] // parts).reshape((-1,) + (1,) * (len(shape) - 1 - position))
    return level


def bell_draw(stream_key, shape, width, limit, shards=(), kind=jnp.bfloat16):
    array = width * jax.random.normal(stream_key, shape, jnp.float32)
    if shards:
        array = array * steps_of(stream_key, shape, shards, -0.22, 0.18)
    return jnp.clip(array, -limit, limit).astype(kind)


def setup_inputs(seed: int = 0) -> dict:
    arg_keys = jax.random.split(jax.random.key(seed), 10)
    checkpoints = bell_draw(arg_keys[0], (STEPS, VARS, LEV, 2, M, M), 0.05, 0.4, ((2, 4), (4, 32)), jnp.float32)
    final_cot = bell_draw(arg_keys[1], (VARS, LEV, 2, M, M), 1.0, 6.0, ((1, 4), (3, 32)), jnp.float32)
    obs_cot = bell_draw(arg_keys[2], (NOBS, VARS, LEV, LAT, LON), 0.03, 0.2, ((3, 32), (4, 4)), jnp.float32)
    obs_time = plant(jax.random.randint(arg_keys[3], (NOBS,), 0, STEPS), jax.random.fold_in(arg_keys[3], 1), 0, STEPS - 1).astype(jnp.int32)
    wave_order = jax.random.permutation(arg_keys[4], M).astype(jnp.int32)
    legendre = bell_draw(arg_keys[5], (M, LAT, M), M ** -0.5, 0.375, ((0, 32),))
    w_in = bell_draw(arg_keys[6], (VARS * LEV, HID), (VARS * LEV) ** -0.5, 0.5)
    w_out = bell_draw(arg_keys[7], (HID, VARS * LEV), HID ** -0.5, 0.25)
    bias = bell_draw(arg_keys[8], (HID,), 0.5, 3.0, (), jnp.float32)
    return dict(checkpoints=checkpoints, final_cot=final_cot, obs_cot=obs_cot, obs_time=obs_time, wave_order=wave_order, legendre=legendre, w_in=w_in, w_out=w_out, bias=bias)


highest = lax.Precision.HIGHEST
dt_scale = 1.0


def lowered(values):
    return lax.optimization_barrier(values.astype(jnp.bfloat16)).astype(jnp.float32)


def tables(wave_order, lon_count):
    longitude = jnp.arange(lon_count, dtype=jnp.int32)
    phase_index = (wave_order[:, None] * longitude[None, :]) % lon_count
    angles = (2.0 * jnp.pi / lon_count) * phase_index.astype(jnp.float32)
    return lowered(jnp.cos(angles)), lowered(jnp.sin(angles))


def synth_legendre(masked, spectral):
    return lowered(jnp.einsum('rjn,vlcrn->vlcrj', masked, lowered(spectral), precision=highest))


def synth_fourier(coefficients, factor, cosine_table, sine_table):
    real_part = coefficients[:, :, 0] * factor[None, None, :, None]
    imag_part = coefficients[:, :, 1] * factor[None, None, :, None]
    return (jnp.einsum('vlrj,ro->vljo', real_part, cosine_table, precision=highest)
            - jnp.einsum('vlrj,ro->vljo', imag_part, sine_table, precision=highest))


def adjoint_fourier(grid_field, factor, cosine_table, sine_table):
    real_part = jnp.einsum('vljo,ro->vlrj', grid_field, cosine_table, precision=highest) * factor[:, None]
    imag_part = -jnp.einsum('vljo,ro->vlrj', grid_field, sine_table, precision=highest) * factor[:, None]
    return lowered(jnp.stack([real_part, imag_part], axis=2))


def adjoint_legendre(masked, coefficients):
    return jnp.einsum('rjn,vlcrj->vlcrn', masked, coefficients, precision=highest)


def reference(checkpoints, final_cot, obs_cot, obs_time, wave_order, legendre, w_in, w_out, bias):
    degrees = jnp.arange(M, dtype=jnp.int32)
    upper_mask = (degrees[None, None, :] >= wave_order[:, None, None]).astype(jnp.float32)
    masked = legendre.astype(jnp.float32) * upper_mask
    cosine_table, sine_table = tables(wave_order, LON)
    weight_m = jnp.where(wave_order == 0, 1.0, 2.0).astype(jnp.float32)
    inverse_lon = jnp.full((M,), 1.0 / LON, jnp.float32)
    degree_float = degrees.astype(jnp.float32)
    damping = 1.0 / (1.0 + 2.0 * degree_float * (degree_float + 1.0) / (M * M))
    feature_count = VARS * LEV
    column_count = LAT * LON
    adjoint = final_cot
    grad_w_in = jnp.zeros((feature_count, HID), jnp.float32)
    grad_w_out = jnp.zeros((HID, feature_count), jnp.float32)
    grad_bias = jnp.zeros((HID,), jnp.float32)
    for step in reversed(range(STEPS)):
        damped = damping * adjoint
        state_grid = synth_fourier(synth_legendre(masked, checkpoints[step]), weight_m, cosine_table, sine_table)
        features = state_grid.astype(jnp.bfloat16).reshape(feature_count, column_count)
        tangent_grid = synth_fourier(synth_legendre(masked, dt_scale * damped), inverse_lon, cosine_table, sine_table)
        tangent = tangent_grid.astype(jnp.bfloat16).reshape(feature_count, column_count)
        preact = jnp.dot(w_in.T, features, preferred_element_type=jnp.float32) + bias[:, None]
        logistic = jax.nn.sigmoid(preact)
        hidden = (preact * logistic).astype(jnp.bfloat16)
        hidden_grad = jnp.dot(w_out, tangent, preferred_element_type=jnp.float32)
        preact_grad = hidden_grad * (logistic * (1.0 + preact * (1.0 - logistic)))
        preact_low = preact_grad.astype(jnp.bfloat16)
        grad_w_out = grad_w_out + jnp.dot(hidden, tangent.T, preferred_element_type=jnp.float32)
        grad_w_in = grad_w_in + jnp.dot(features, preact_low.T, preferred_element_type=jnp.float32)
        grad_bias = grad_bias + jnp.sum(preact_grad, axis=1)
        column_grad = jnp.dot(w_in, preact_low, preferred_element_type=jnp.float32).reshape(VARS, LEV, LAT, LON)
        obs_weight = (obs_time == step).astype(jnp.float32)
        column_grad = column_grad + jnp.einsum('i,ivljo->vljo', obs_weight, obs_cot, precision=highest)
        back = adjoint_fourier(lowered(column_grad), weight_m, cosine_table, sine_table)
        adjoint = damped + adjoint_legendre(masked, back)
    return adjoint, grad_w_in, grad_w_out, grad_bias
```

```python
import functools

import jax
import jax.numpy as jnp
import numpy as np
from jax import lax
from jax.experimental import pallas as pl
from jax.experimental.pallas import tpu as pltpu
from jax.sharding import Mesh
from jax.sharding import PartitionSpec as P

BAND = ("band_0", "band_1", "band_2")
ALL = ("band_0", "band_1", "band_2", "lev")
F32 = jnp.float32
BF16 = jnp.bfloat16

RHO = 8
N = 256
LON = 512
FEAT = 128
HID = 512
STEPS = 4
VL = 32
DEV = 128


def mm(a, b):
    return jnp.dot(a, b, preferred_element_type=F32)


def mm_nt(a, b):
    return lax.dot_general(a, b, (((1,), (1,)), ((), ())), preferred_element_type=F32)


def lane_of(rows, lanes):
    return lax.broadcasted_iota(jnp.int32, (rows, lanes), 1)


def damping_row():
    n = lane_of(1, N).astype(F32)
    return 1.0 / (1.0 + 2.0 * n * (n + 1.0) / (N * N))


def halve(ref, halves):
    for h in range(2):
        halves[h] = ref[:, h * 128 : (h + 1) * 128]


def strided_rows(halves, rho):
    return jnp.concatenate(
        [
            jnp.concatenate(
                [halves[h, pl.ds(p * RHO + rho, VL, stride=2 * RHO), :] for h in range(2)], axis=1
            )
            for p in range(2)
        ],
        axis=0,
    )


def tangent_scale(m):
    return jnp.where(m == 0, 1.0 / LON, 0.5 / LON).astype(F32)


def synth_rho(table, tangent, state, rho, rows_t, rows_s):
    parts = []
    for s in (tangent, state):
        s = s.astype(BF16)
        parts += [s[:VL], s[:VL], s[VL:], s[VL:]]
    sums = mm_nt(table, jnp.concatenate(parts, axis=0))
    even = (lane_of(DEV, 2 * DEV) // VL) % 2 == 0
    both = jnp.where(even, sums[:DEV], sums[DEV:])
    rows_t[pl.ds(rho, DEV, stride=RHO), :] = both[:, :DEV]
    rows_s[pl.ds(rho, DEV, stride=RHO), :] = both[:, DEV:]


def write_chunks(send, rows_t, rows_s):
    send[:, 0] = rows_t[...].reshape(DEV, RHO, 128).astype(BF16)
    send[:, 1] = rows_s[...].reshape(DEV, RHO, 128).astype(BF16)


def first_kernel(
    waves, legendre, final, state, send, damped, table, tall, rows_t, rows_s, final_rows, state_rows
):
    damping = damping_row()
    halve(final, final_rows)
    halve(state.at[0], state_rows)
    degree = lane_of(N, N)
    for rho in range(RHO):
        m = waves[rho]
        kept = jnp.where(degree >= m, legendre[rho].astype(F32), 0.0)
        for h in range(2):
            tall[h] = kept[:, h * 128 : (h + 1) * 128]
        for jj in range(2):
            for h in range(2):
                part = tall[h, pl.ds(jj, DEV, stride=2), :].astype(BF16)
                table[rho, jj * DEV : (jj + 1) * DEV, h * 128 : (h + 1) * 128] = part
        now = damping * strided_rows(final_rows, rho)
        damped[rho] = now
        synth_rho(
            table[rho], now * tangent_scale(m), strided_rows(state_rows, rho), rho, rows_t, rows_s
        )
    write_chunks(send, rows_t, rows_s)


def adjoint_rho(rows, table, rho):
    back = rows[pl.ds(rho, DEV, stride=RHO), :].T
    halves = []
    for p in range(2):
        at = 2 * p * VL
        halves.append(jnp.concatenate([back[at : at + VL], back[at + VL : at + 2 * VL]], axis=1))
    return mm(jnp.concatenate(halves, axis=0).astype(BF16), table)


def turn_kernel(waves, back, damped_in, table, state, send, damped, rows, rows_t, rows_s, state_rows):
    damping = damping_row()
    halve(state.at[0], state_rows)
    rows[...] = back[...].astype(F32).reshape(DEV * RHO, 128)
    for rho in range(RHO):
        now = damping * (damped_in[rho] + adjoint_rho(rows, table[rho], rho))
        damped[rho] = now
        synth_rho(
            table[rho],
            now * tangent_scale(waves[rho]),
            strided_rows(state_rows, rho),
            rho,
            rows_t,
            rows_s,
        )
    write_chunks(send, rows_t, rows_s)


def last_kernel(back, damped_in, table, out, rows, out_rows):
    rows[...] = back[:, 0].astype(F32).reshape(DEV * RHO, 128)
    for rho in range(RHO):
        now = damped_in[rho] + adjoint_rho(rows, table[rho], rho)
        for p in range(2):
            for h in range(2):
                part = now[p * VL : (p + 1) * VL, h * 128 : (h + 1) * 128]
                out_rows[h, pl.ds(p * RHO + rho, VL, stride=2 * RHO), :] = part
    for h in range(2):
        out[:, h * 128 : (h + 1) * 128] = out_rows[h]


def share_kernel(back, bias_part, send):
    total = jnp.sum(back[:, 1].astype(F32), axis=0)
    send[:, 0] = jnp.broadcast_to(total[None], (DEV, 8, 128)).astype(BF16)
    send[:, 1] = jnp.broadcast_to(bias_part[...][None], (DEV, 8, 128)).astype(BF16)


def ending_kernel(parts, w_in_out, w_out_out, bias_out):
    rows = parts[:, 0].astype(F32).reshape(2 * HID, 128)
    w_in_out[...] = rows[:HID].T
    w_out_out[...] = rows[HID:]
    total = jnp.sum(parts[:, 1].astype(F32), axis=0)
    bias_out[...] = total[:4] + total[4:]


def tables_kernel(waves, base, w_in, bias, trig, w_in_t, bias_wide):
    m = lax.broadcasted_iota(jnp.int32, (N, N), 0)
    weight = jnp.where(m == 0, 1.0, 2.0).astype(F32)
    pick = jnp.where(m == waves[...], weight, 0.0).T.astype(BF16)
    both = mm(pick, base[...]).astype(BF16)
    trig[:N] = both[:, :LON]
    trig[N:] = both[:, LON:]
    w_in_t[...] = w_in[...].astype(F32).T.astype(BF16)
    bias_wide[...] = jnp.broadcast_to(bias[...], (128, HID)).T


def obs_kernel(obs_time, obs, out):
    for j in range(8):
        pieces = [obs[i, pl.ds(j, FEAT, stride=8), :] for i in range(4)]
        for step in range(STEPS):
            total = jnp.zeros((FEAT, 128), F32)
            for i in range(4):
                total += jnp.where(obs_time[i] == step, 1.0, 0.0).astype(F32) * pieces[i]
            out[j // 2, step, j % 2] = total.astype(BF16)


def column_kernel(first, last, *refs):
    got, trig, w_in, w_in_t, w_out, bias, obs = refs[:7]
    refs = refs[7:]
    if not first:
        acc_in, accb_in = refs[:2]
        refs = refs[2:]
    send = refs[0]
    if last:
        bias_part = refs[1]
        acc, accb, turned, grid, grads = refs[2:]
    else:
        acc, accb, turned, grid, grads = refs[1:]
    for kind in range(2):
        for y in range(4):
            x = got[:, y, kind].astype(F32).reshape(N, 128).T.astype(BF16)
            for p in range(2):
                for jj in range(2):
                    at = (2 * p + jj) * VL
                    turned[kind, jj, y * VL : (y + 1) * VL, p * N : (p + 1) * N] = x[at : at + VL]
    for kind in range(2):
        for jj in range(2):
            g = mm(turned[kind, jj], trig[...])
            g = jnp.concatenate(
                [g[(y * 4 + v) * 8 : (y * 4 + v + 1) * 8] for v in range(4) for y in range(4)], axis=0
            ).astype(BF16)
            for half in range(2):
                grid[kind, 2 * jj + half] = g[:, half * 256 : (half + 1) * 256]
    if first:
        acc[...] = jnp.zeros_like(acc)
        accb[...] = jnp.zeros_like(accb)
    else:
        acc[...] = acc_in[...]
        accb[...] = accb_in[...]

    def block(cb, carry):
        tangent = grid[0, cb]
        features = grid[1, cb]
        back = jnp.zeros((FEAT, 256), F32)
        for hb in range(2):
            rows = slice(hb * 256, (hb + 1) * 256)
            wide = bias[rows, :]
            pre = mm(w_in_t[rows, :], features) + jnp.concatenate([wide, wide], axis=1)
            logistic = 0.5 * jnp.tanh(0.5 * pre) + 0.5
            hidden = (pre * logistic).astype(BF16)
            pre_grad = mm(w_out[rows, :], tangent) * (logistic * (1.0 + pre * (1.0 - logistic)))
            low = pre_grad.astype(BF16)
            acc[rows, :] += mm_nt(low, features)
            acc[hb * 256 + HID : (hb + 1) * 256 + HID, :] += mm_nt(hidden, tangent)
            accb[rows, :] += pre_grad[:, :128] + pre_grad[:, 128:]
            back += mm(w_in[:, rows], low)
        jj = cb // 2
        half = cb % 2
        seen = jnp.concatenate([obs[2 * half + k, 0, jj] for k in range(2)], axis=1)
        back += seen.astype(F32)
        back = jnp.concatenate(
            [back[(v * 4 + y) * 8 : (v * 4 + y + 1) * 8] for y in range(4) for v in range(4)], axis=0
        )
        grads[jj, half] = back.astype(BF16)
        return carry

    lax.fori_loop(0, 4, block, 0)

    real = (lane_of(N, 2 * 128) // 64) % 2 == 0
    for pair in range(2):
        rows = []
        for y in (2 * pair, 2 * pair + 1):
            for p in range(2):
                for jj in range(2):
                    rows.append(
                        jnp.concatenate(
                            [grads[jj, half, y * VL : (y + 1) * VL, :] for half in range(2)], axis=1
                        )
                    )
        rows = jnp.concatenate(rows, axis=0)
        mixed = jnp.where(real, mm_nt(trig[:N], rows), mm_nt(trig[N:], rows))
        for k in range(2):
            chunk = mixed[:, k * 128 : (k + 1) * 128].reshape(32, 8, 128).astype(BF16)
            if last:
                send[:, 2 * pair + k, 0] = chunk
            else:
                send[:, 2 * pair + k] = chunk
    if last:
        send[:, :, 1] = acc[...].reshape(32, 4, 8, 128).astype(BF16)
        ones = jnp.ones((8, 128), F32)
        sums = lax.dot_general(
            ones,
            accb[...],
            (((1,), (1,)), ((), ())),
            preferred_element_type=F32,
            precision=lax.Precision.HIGHEST,
        )
        for k in range(4):
            part = sums[:1, k * 128 : (k + 1) * 128]
            high = part.astype(BF16).astype(F32)
            bias_part[k : k + 1, :] = high
            bias_part[k + 4 : k + 5, :] = part - high


VMEM = pl.BlockSpec(memory_space=pltpu.VMEM)
SMEM = pl.BlockSpec(memory_space=pltpu.SMEM)


def shape(dims, kind):
    return jax.ShapeDtypeStruct(dims, kind)


def cost(flops, nbytes):
    return pl.CostEstimate(flops=flops, bytes_accessed=nbytes, transcendentals=0)


def state_spec(step):
    return pl.BlockSpec((1, 512, N), lambda i: (step, 0, 0))


def whole(dims):
    return pl.BlockSpec(dims, lambda i: (0,) * len(dims))


def call(body, ins, outs, scratch, in_specs, name, flops, nbytes):
    many = isinstance(outs, (list, tuple))
    outs_list = list(outs) if many else [outs]
    out_specs = [whole(o.shape) for o in outs_list]
    return pl.pallas_call(
        body,
        grid=(1,),
        out_shape=outs_list if many else outs,
        in_specs=in_specs,
        out_specs=out_specs if many else out_specs[0],
        scratch_shapes=scratch,
        cost_estimate=cost(flops, nbytes),
        name=name,
    )(*ins)


def exchange(array, axes):
    return lax.all_to_all(array, axes, split_axis=0, concat_axis=0, tiled=True)


def trig_base():
    phase = (np.arange(N)[:, None] * np.arange(LON)[None, :]) % LON
    angle = 2.0 * np.pi / LON * phase
    return jnp.asarray(np.concatenate([np.cos(angle), -np.sin(angle)], axis=1), BF16)


def shards(checkpoints, final_cot, obs_cot, obs_time, wave_order, legendre, w_in, w_out, bias):
    waves = lax.dynamic_slice_in_dim(wave_order, lax.axis_index(BAND) * RHO, RHO)
    states = checkpoints.reshape(STEPS, 512, N)
    final = final_cot.reshape(512, N)
    seen = obs_cot.reshape(4, FEAT * 8, 128)
    chunks = shape((DEV, 2, RHO, 128), BF16)
    tall = pltpu.VMEM((DEV * RHO, 128), F32)
    halves = pltpu.VMEM((2, 512, 128), F32)

    send, damped, table = call(
        first_kernel,
        (waves, legendre, final, states),
        (chunks, shape((RHO, 64, N), F32), shape((RHO, N, N), BF16)),
        [pltpu.VMEM((2, N, 128), F32), tall, tall, halves, halves],
        [SMEM, whole(legendre.shape), whole(final.shape), state_spec(STEPS - 1)],
        "first",
        300_000_000,
        4_000_000,
    )
    trig, w_in_t, bias_wide = call(
        tables_kernel,
        (wave_order.reshape(1, N), trig_base(), w_in, bias.reshape(1, HID)),
        (shape((2 * N, LON), BF16), shape((HID, FEAT), BF16), shape((HID, 128), F32)),
        [],
        [whole((1, N)), whole((N, 2 * LON)), whole(w_in.shape), whole((1, HID))],
        "tables",
        140_000_000,
        1_500_000,
    )
    obs_parts = call(
        obs_kernel,
        (obs_time, seen),
        shape((4, STEPS, 2, FEAT, 128), BF16),
        [],
        [SMEM, whole(seen.shape)],
        "obs",
        10_000_000,
        3_000_000,
    )
    obs_cols = exchange(obs_parts, ("lev",))

    sums = ()
    for step in reversed(range(STEPS)):
        first = step == STEPS - 1
        last = step == 0
        got = exchange(send, ALL).reshape(32, 4, 2, RHO, 128)
        acc_shapes = [shape((2 * HID, 128), F32), shape((HID, 128), F32)]
        scratch = [
            pltpu.VMEM((2, 2, FEAT, 2 * N), BF16),
            pltpu.VMEM((2, 4, FEAT, 256), BF16),
            pltpu.VMEM((2, 2, FEAT, 256), BF16),
        ]
        if last:
            outs = [shape((32, 4, 2, RHO, 128), BF16), shape((8, 128), F32)]
            scratch = [pltpu.VMEM(a.shape, F32) for a in acc_shapes] + scratch
        else:
            outs = [shape((32, 4, RHO, 128), BF16)] + acc_shapes
        ins = (got, trig, w_in, w_in_t, w_out, bias_wide, obs_cols) + tuple(sums)
        specs = [whole(a.shape) for a in ins]
        specs[6] = pl.BlockSpec((4, 1, 2, FEAT, 128), functools.partial(lambda s, i: (0, s, 0, 0, 0), step))
        back, *sums = call(
            functools.partial(column_kernel, first, last),
            ins,
            outs,
            scratch,
            specs,
            f"columns_{step}",
            1_200_000_000,
            3_000_000,
        )
        if not last:
            back = exchange(back.reshape(DEV, RHO, 128), ALL)
            send, damped = call(
                turn_kernel,
                (waves, back, damped, table, states),
                (chunks, shape((RHO, 64, N), F32)),
                [tall, tall, tall, halves],
                [SMEM, whole(back.shape), whole(damped.shape), whole(table.shape), state_spec(step - 1)],
                f"turn_{step}",
                400_000_000,
                4_000_000,
            )
    back = exchange(back.reshape(DEV, 2, RHO, 128), ALL)
    (bias_part,) = sums
    parts = call(
        share_kernel,
        (back, bias_part),
        chunks,
        [],
        [whole(back.shape), whole(bias_part.shape)],
        "share",
        1_000_000,
        1_000_000,
    )
    parts = exchange(parts, ALL)
    adjoint = call(
        last_kernel,
        (back, damped, table),
        shape((512, N), F32),
        [tall, halves],
        [whole(back.shape), whole(damped.shape), whole(table.shape)],
        "last",
        100_000_000,
        3_000_000,
    )
    grad_w_in, grad_w_out, grad_bias = call(
        ending_kernel,
        (parts,),
        (shape((FEAT, HID), F32), shape((HID, FEAT), F32), shape((4, 128), F32)),
        [],
        [whole(parts.shape)],
        "ending",
        1_000_000,
        1_500_000,
    )
    return (adjoint.reshape(final_cot.shape), grad_w_in, grad_w_out, grad_bias.reshape(HID))


def solution(mesh):
    torus = Mesh(mesh.devices.reshape(4, 4, 2, mesh.shape["lev"]), ("band_0", "band_1", "band_2", "lev"))
    placed = (
        P(None, None, "lev", None, BAND, None),
        P(None, "lev", None, BAND, None),
        P(None, None, None, BAND, "lev"),
        P(),
        P(),
        P(BAND, None, None),
        P(),
        P(),
        P(),
    )
    return jax.shard_map(
        shards,
        mesh=torus,
        in_specs=placed,
        out_specs=(P(None, "lev", None, BAND, None), P(), P(), P()),
        check_vma=False,
    )
```

```python
import functools

import jax
import jax.numpy as jnp
import numpy as np
from jax import lax
from jax.experimental import pallas as pl
from jax.experimental.pallas import tpu as pltpu
from jax.sharding import Mesh
from jax.sharding import PartitionSpec as P

BAND = ("band_0", "band_1", "band_2")
ALL = ("band_0", "band_1", "band_2", "lev")
F32 = jnp.float32
BF16 = jnp.bfloat16

RHO = 8
N = 256
LON = 512
FEAT = 128
HID = 512
STEPS = 4
VL = 32
DEV = 128


def mm(a, b):
    return jnp.dot(a, b, preferred_element_type=F32)


def mm_nt(a, b):
    return lax.dot_general(a, b, (((1,), (1,)), ((), ())), preferred_element_type=F32)


def lane_of(rows, lanes):
    return lax.broadcasted_iota(jnp.int32, (rows, lanes), 1)


def damping_row():
    n = lane_of(1, N).astype(F32)
    return 1.0 / (1.0 + 2.0 * n * (n + 1.0) / (N * N))


def halve(ref, halves):
    for h in range(2):
        halves[h] = ref[:, h * 128 : (h + 1) * 128]


def strided_rows(halves, rho):
    return jnp.concatenate(
        [
            jnp.concatenate(
                [halves[h, pl.ds(p * RHO + rho, VL, stride=2 * RHO), :] for h in range(2)], axis=1
            )
            for p in range(2)
        ],
        axis=0,
    )


def tangent_scale(m):
    return jnp.where(m == 0, 1.0 / LON, 0.5 / LON).astype(F32)


def synth_rho(table, tangent, state, rho, rows_t, rows_s):
    parts = []
    for s in (tangent, state):
        s = s.astype(BF16)
        parts += [s[:VL], s[:VL], s[VL:], s[VL:]]
    sums = mm_nt(table, jnp.concatenate(parts, axis=0))
    even = (lane_of(DEV, 2 * DEV) // VL) % 2 == 0
    both = jnp.where(even, sums[:DEV], sums[DEV:])
    rows_t[pl.ds(rho, DEV, stride=RHO), :] = both[:, :DEV]
    rows_s[pl.ds(rho, DEV, stride=RHO), :] = both[:, DEV:]


def write_chunks(send, rows_t, rows_s):
    send[:, 0] = rows_t[...].reshape(DEV, RHO, 128).astype(BF16)
    send[:, 1] = rows_s[...].reshape(DEV, RHO, 128).astype(BF16)


def first_kernel(
    waves, legendre, final, state, send, damped, table, tall, rows_t, rows_s, final_rows, state_rows
):
    damping = damping_row()
    band = lax.axis_index(BAND)
    halve(final, final_rows)
    halve(state.at[0], state_rows)
    degree = lane_of(N, N)
    for rho in range(RHO):
        m = waves[band * RHO + rho]
        kept = jnp.where(degree >= m, legendre[rho].astype(F32), 0.0)
        for h in range(2):
            tall[h] = kept[:, h * 128 : (h + 1) * 128]
        for jj in range(2):
            for h in range(2):
                part = tall[h, pl.ds(jj, DEV, stride=2), :].astype(BF16)
                table[rho, jj * DEV : (jj + 1) * DEV, h * 128 : (h + 1) * 128] = part
        now = damping * strided_rows(final_rows, rho)
        damped[rho] = now
        synth_rho(
            table[rho], now * tangent_scale(m), strided_rows(state_rows, rho), rho, rows_t, rows_s
        )
    write_chunks(send, rows_t, rows_s)


def adjoint_rho(rows, table, rho):
    back = rows[pl.ds(rho, DEV, stride=RHO), :].T
    halves = []
    for p in range(2):
        at = 2 * p * VL
        halves.append(jnp.concatenate([back[at : at + VL], back[at + VL : at + 2 * VL]], axis=1))
    return mm(jnp.concatenate(halves, axis=0).astype(BF16), table)


def turn_kernel(
    step,
    waves,
    back,
    damped_in,
    table,
    states_hbm,
    send,
    damped,
    rows,
    rows_t,
    rows_s,
    state_rows,
    state,
    sem,
):
    copy = pltpu.make_async_copy(states_hbm.at[step], state, sem)
    copy.start()
    damping = damping_row()
    band = lax.axis_index(BAND)
    rows[...] = back[...].astype(F32).reshape(DEV * RHO, 128)
    copy.wait()
    halve(state, state_rows)
    for rho in range(RHO):
        now = damping * (damped_in[rho] + adjoint_rho(rows, table[rho], rho))
        damped[rho] = now
        synth_rho(
            table[rho],
            now * tangent_scale(waves[band * RHO + rho]),
            strided_rows(state_rows, rho),
            rho,
            rows_t,
            rows_s,
        )
    write_chunks(send, rows_t, rows_s)


def last_kernel(back, damped_in, table, out, rows, out_rows):
    rows[...] = back[:, 0].astype(F32).reshape(DEV * RHO, 128)
    for rho in range(RHO):
        now = damped_in[rho] + adjoint_rho(rows, table[rho], rho)
        for p in range(2):
            for h in range(2):
                part = now[p * VL : (p + 1) * VL, h * 128 : (h + 1) * 128]
                out_rows[h, pl.ds(p * RHO + rho, VL, stride=2 * RHO), :] = part
    for h in range(2):
        out[:, h * 128 : (h + 1) * 128] = out_rows[h]


def share_kernel(back, bias_part, send):
    total = jnp.sum(back[:, 1].astype(F32), axis=0)
    send[:, 0] = jnp.broadcast_to(total[None], (DEV, 8, 128)).astype(BF16)
    send[:, 1] = jnp.broadcast_to(bias_part[...][None], (DEV, 8, 128)).astype(BF16)


def ending_kernel(parts, w_in_out, w_out_out, bias_out):
    rows = parts[:, 0].astype(F32).reshape(2 * HID, 128)
    w_in_out[...] = rows[:HID].T
    w_out_out[...] = rows[HID:]
    total = jnp.sum(parts[:, 1].astype(F32), axis=0)
    bias_out[...] = total[:4] + total[4:]


def tables_kernel(waves, base, w_in, bias, trig, w_in_t, bias_wide):
    m = lax.broadcasted_iota(jnp.int32, (N, N), 0)
    weight = jnp.where(m == 0, 1.0, 2.0).astype(F32)
    pick = jnp.where(m == waves[...], weight, 0.0).T.astype(BF16)
    both = mm(pick, base[...]).astype(BF16)
    trig[:N] = both[:, :LON]
    trig[N:] = both[:, LON:]
    w_in_t[...] = w_in[...].astype(F32).T.astype(BF16)
    bias_wide[...] = jnp.broadcast_to(bias[...], (128, HID)).T


def obs_kernel(obs_time, obs, *outs):
    lev = lax.axis_index("lev")
    for k in range(4):
        to = lax.rem(lev + k, 4)
        for jj in range(2):
            pieces = [obs[i, pl.ds(2 * to + jj, FEAT, stride=8), :] for i in range(4)]
            for step in range(STEPS):
                total = jnp.zeros((FEAT, 128), F32)
                for i in range(4):
                    total += jnp.where(obs_time[i] == step, 1.0, 0.0).astype(F32) * pieces[i]
                if step == STEPS - 1:
                    outs[k][0, jj] = total.astype(BF16)
                else:
                    outs[4 + k][step, jj] = total.astype(BF16)


def column_kernel(first, last, step, *refs):
    got, trig, w_in, w_in_t, w_out, bias = refs[:6]
    obs_parts = refs[6:10]
    refs = refs[10:]
    if not first:
        acc_in, accb_in = refs[:2]
        refs = refs[2:]
    send = refs[0]
    if last:
        bias_part = refs[1]
        acc, accb, turned, grid, grads, obs, sems = refs[2:]
    else:
        acc, accb, turned, grid, grads, obs, sems = refs[1:]
    lev = lax.axis_index("lev")
    copies = [
        pltpu.make_async_copy(obs_parts[k].at[step], obs.at[lax.rem(lev + 4 - k, 4)], sems.at[k])
        for k in range(4)
    ]
    for copy in copies:
        copy.start()
    for kind in range(2):
        for y in range(4):
            x = got[:, y, kind].reshape(N, 128).T
            for p in range(2):
                for jj in range(2):
                    at = (2 * p + jj) * VL
                    turned[kind, jj, y * VL : (y + 1) * VL, p * N : (p + 1) * N] = x[at : at + VL]
    for kind in range(2):
        for jj in range(2):
            g = mm(turned[kind, jj], trig[...])
            g = jnp.concatenate(
                [g[(y * 4 + v) * 8 : (y * 4 + v + 1) * 8] for v in range(4) for y in range(4)], axis=0
            ).astype(BF16)
            for half in range(2):
                grid[kind, 2 * jj + half] = g[:, half * 256 : (half + 1) * 256]
    if first:
        acc[...] = jnp.zeros_like(acc)
        accb[...] = jnp.zeros_like(accb)
    else:
        acc[...] = acc_in[...]
        accb[...] = accb_in[...]

    for copy in copies:
        copy.wait()

    def block(cb, carry):
        tangent = grid[0, cb]
        features = grid[1, cb]
        back = jnp.zeros((FEAT, 256), F32)
        for hb in range(2):
            rows = slice(hb * 256, (hb + 1) * 256)
            wide = bias[rows, :]
            pre = mm(w_in_t[rows, :], features) + jnp.concatenate([wide, wide], axis=1)
            logistic = 0.5 * jnp.tanh(0.5 * pre) + 0.5
            hidden = (pre * logistic).astype(BF16)
            pre_grad = mm(w_out[rows, :], tangent) * (logistic * (1.0 + pre * (1.0 - logistic)))
            low = pre_grad.astype(BF16)
            acc[rows, :] += mm_nt(low, features)
            acc[hb * 256 + HID : (hb + 1) * 256 + HID, :] += mm_nt(hidden, tangent)
            accb[rows, :] += pre_grad[:, :128] + pre_grad[:, 128:]
            back += mm(w_in[:, rows], low)
        jj = cb // 2
        half = cb % 2
        seen = jnp.concatenate([obs[2 * half + k, jj] for k in range(2)], axis=1)
        back += seen.astype(F32)
        back = jnp.concatenate(
            [back[(v * 4 + y) * 8 : (v * 4 + y + 1) * 8] for y in range(4) for v in range(4)], axis=0
        )
        grads[jj, half] = back.astype(BF16)
        return carry

    lax.fori_loop(0, 4, block, 0, unroll=True)

    real = (lane_of(N, 2 * 128) // 64) % 2 == 0
    for pair in range(2):
        rows = []
        for y in (2 * pair, 2 * pair + 1):
            for _ in range(2):
                for jj in range(2):
                    rows.append(
                        jnp.concatenate(
                            [grads[jj, half, y * VL : (y + 1) * VL, :] for half in range(2)], axis=1
                        )
                    )
        rows = jnp.concatenate(rows, axis=0)
        mixed = jnp.where(real, mm_nt(trig[:N], rows), mm_nt(trig[N:], rows))
        for k in range(2):
            chunk = mixed[:, k * 128 : (k + 1) * 128].reshape(32, 8, 128).astype(BF16)
            if last:
                send[:, 2 * pair + k, 0] = chunk
            else:
                send[:, 2 * pair + k] = chunk
    if last:
        send[:, :, 1] = acc[...].reshape(32, 4, 8, 128).astype(BF16)
        ones = jnp.ones((8, 128), F32)
        sums = lax.dot_general(
            ones,
            accb[...],
            (((1,), (1,)), ((), ())),
            preferred_element_type=F32,
            precision=lax.Precision.HIGHEST,
        )
        for k in range(4):
            part = sums[:1, k * 128 : (k + 1) * 128]
            high = part.astype(BF16).astype(F32)
            bias_part[k : k + 1, :] = high
            bias_part[k + 4 : k + 5, :] = part - high


VMEM = pl.BlockSpec(memory_space=pltpu.VMEM)
SMEM = pl.BlockSpec(memory_space=pltpu.SMEM)
HBM = pl.BlockSpec(memory_space=pltpu.HBM)


def shape(dims, kind):
    return jax.ShapeDtypeStruct(dims, kind)


def cost(flops, nbytes):
    return pl.CostEstimate(flops=flops, bytes_accessed=nbytes, transcendentals=0)


def whole(dims):
    return pl.BlockSpec(dims, lambda i: (0,) * len(dims))


VMEM_LIMIT = 20 * 1024 * 1024
BIG = 63_000_000


def call(body, ins, outs, scratch, in_specs, flops, nbytes, vmem=VMEM_LIMIT):
    many = isinstance(outs, (list, tuple))
    outs_list = list(outs) if many else [outs]
    out_specs = [whole(o.shape) for o in outs_list]
    return pl.pallas_call(
        body,
        grid=(1,),
        out_shape=outs_list if many else outs,
        in_specs=in_specs,
        out_specs=out_specs if many else out_specs[0],
        scratch_shapes=scratch,
        cost_estimate=cost(flops, nbytes),
        compiler_params=pltpu.CompilerParams(vmem_limit_bytes=vmem),
    )(*ins)


def exchange(array, axes):
    return lax.all_to_all(array, axes, split_axis=0, concat_axis=0, tiled=True)


def trig_base():
    phase = (np.arange(N)[:, None] * np.arange(LON)[None, :]) % LON
    angle = 2.0 * np.pi / LON * phase
    return jnp.asarray(np.concatenate([np.cos(angle), -np.sin(angle)], axis=1), BF16)


def program(checkpoints, final_cot, obs_cot, obs_time, wave_order, legendre, w_in, w_out, bias):
    states = checkpoints.reshape(STEPS, 512, N)
    final = final_cot.reshape(512, N)
    seen = obs_cot.reshape(4, FEAT * 8, 128)
    state_spec = pl.BlockSpec((1, 512, N), lambda i: (STEPS - 1, 0, 0))
    chunks = shape((DEV, 2, RHO, 128), BF16)
    tall = pltpu.VMEM((DEV * RHO, 128), F32)
    halves = pltpu.VMEM((2, 512, 128), F32)

    send, damped, table = call(
        first_kernel,
        (wave_order, legendre, final, states),
        (chunks, shape((RHO, 64, N), F32), shape((RHO, N, N), BF16)),
        [
            pltpu.VMEM((2, N, 128), F32),
            tall,
            tall,
            halves,
            halves,
        ],
        [SMEM, whole(legendre.shape), whole(final.shape), state_spec],
        300_000_000,
        4_000_000,
        BIG,
    )
    trig, w_in_t, bias_wide = call(
        tables_kernel,
        (wave_order.reshape(1, N), trig_base(), w_in, bias.reshape(1, HID)),
        (shape((2 * N, LON), BF16), shape((HID, FEAT), BF16), shape((HID, 128), F32)),
        [],
        [whole((1, N)), whole((N, 2 * LON)), whole(w_in.shape), whole((1, HID))],
        140_000_000,
        1_500_000,
        BIG,
    )
    obs_parts = call(
        obs_kernel,
        (obs_time, seen),
        [shape((1, 2, FEAT, 128), BF16)] * 4 + [shape((STEPS - 1, 2, FEAT, 128), BF16)] * 4,
        [],
        [SMEM, whole(seen.shape)],
        10_000_000,
        3_000_000,
        BIG,
    )
    obs_cols = []
    for k, part in enumerate(obs_parts):
        if k % 4:
            part = lax.ppermute(part, "lev", [(i, (i + k) % 4) for i in range(4)])
        obs_cols.append(part)

    sums = ()
    for step in reversed(range(STEPS)):
        first = step == STEPS - 1
        last = step == 0
        got = exchange(send, ALL).reshape(32, 4, 2, RHO, 128)
        acc_shapes = [shape((2 * HID, 128), F32), shape((HID, 128), F32)]
        scratch = [
            pltpu.VMEM((2, 2, FEAT, 2 * N), BF16),
            pltpu.VMEM((2, 4, FEAT, 256), BF16),
            pltpu.VMEM((2, 2, FEAT, 256), BF16),
            pltpu.VMEM((4, 2, FEAT, 128), BF16),
            pltpu.SemaphoreType.DMA((4,)),
        ]
        if last:
            outs = [shape((32, 4, 2, RHO, 128), BF16), shape((8, 128), F32)]
            scratch = [pltpu.VMEM(a.shape, F32) for a in acc_shapes] + scratch
        else:
            outs = [shape((32, 4, RHO, 128), BF16)] + acc_shapes
        obs_now = obs_cols[:4] if first else obs_cols[4:]
        ins = (got, trig, w_in, w_in_t, w_out, bias_wide, *obs_now) + tuple(sums)
        specs = [whole(a.shape) for a in ins]
        for k in range(4):
            specs[6 + k] = HBM
        back, *sums = call(
            functools.partial(column_kernel, first, last, step % (STEPS - 1)),
            ins,
            outs,
            scratch,
            specs,
            1_200_000_000,
            3_000_000,
            BIG if first else VMEM_LIMIT,
        )
        if not last:
            back = exchange(back.reshape(DEV, RHO, 128), ALL)
            send, damped = call(
                functools.partial(turn_kernel, step - 1),
                (wave_order, back, damped, table, states),
                (chunks, shape((RHO, 64, N), F32)),
                [tall, tall, tall, halves, pltpu.VMEM(final.shape, F32), pltpu.SemaphoreType.DMA],
                [SMEM, whole(back.shape), whole(damped.shape), whole(table.shape), HBM],
                400_000_000,
                4_000_000,
            )
    back = exchange(back.reshape(DEV, 2, RHO, 128), ALL)
    (bias_part,) = sums
    parts = call(
        share_kernel,
        (back, bias_part),
        chunks,
        [],
        [whole(back.shape), whole(bias_part.shape)],
        1_000_000,
        1_000_000,
    )
    parts = exchange(parts, ALL)
    adjoint = call(
        last_kernel,
        (back, damped, table),
        shape((512, N), F32),
        [tall, halves],
        [whole(back.shape), whole(damped.shape), whole(table.shape)],
        100_000_000,
        3_000_000,
    )
    grad_w_in, grad_w_out, grad_bias = call(
        ending_kernel,
        (parts,),
        (shape((FEAT, HID), F32), shape((HID, FEAT), F32), shape((4, 128), F32)),
        [],
        [whole(parts.shape)],
        1_000_000,
        1_500_000,
    )
    return (adjoint.reshape(final_cot.shape), grad_w_in, grad_w_out, grad_bias.reshape(HID))


def solution(mesh):
    torus = Mesh(mesh.devices.reshape(4, 4, 2, mesh.shape["lev"]), ("band_0", "band_1", "band_2", "lev"))
    placed = (
        P(None, None, "lev", None, BAND, None),
        P(None, "lev", None, BAND, None),
        P(None, None, None, BAND, "lev"),
        P(),
        P(),
        P(BAND, None, None),
        P(),
        P(),
        P(),
    )
    return jax.shard_map(
        program,
        mesh=torus,
        in_specs=placed,
        out_specs=(P(None, "lev", None, BAND, None), P(), P(), P()),
        check_vma=False,
    )
```

```python
import functools

import jax
import jax.numpy as jnp
import numpy as np
from jax import lax
from jax.experimental import pallas as pl
from jax.experimental.pallas import tpu as pltpu
from jax.sharding import Mesh
from jax.sharding import PartitionSpec as P

BAND = ("band_0", "band_1", "band_2")
ALL = ("band_0", "band_1", "band_2", "lev")
F32 = jnp.float32
BF16 = jnp.bfloat16

RHO = 8
N = 256
LON = 512
FEAT = 128
HID = 512
STEPS = 4
VL = 32
DEV = 128


def mm(a, b):
    return jnp.dot(a, b, preferred_element_type=F32)


def mm_nt(a, b):
    return lax.dot_general(a, b, (((1,), (1,)), ((), ())), preferred_element_type=F32)


def lane_of(rows, lanes):
    return lax.broadcasted_iota(jnp.int32, (rows, lanes), 1)


def damping_row():
    n = lane_of(1, N).astype(F32)
    return 1.0 / (1.0 + 2.0 * n * (n + 1.0) / (N * N))


def halve(ref, halves):
    for h in range(2):
        halves[h] = ref[:, h * 128 : (h + 1) * 128]


def strided_rows(halves, rho):
    return jnp.concatenate(
        [
            jnp.concatenate(
                [halves[h, pl.ds(p * RHO + rho, VL, stride=2 * RHO), :] for h in range(2)], axis=1
            )
            for p in range(2)
        ],
        axis=0,
    )


def tangent_scale(m):
    return jnp.where(m == 0, 1.0 / LON, 0.5 / LON).astype(F32)


def synth_rho(table, tangent, state, rho, rows_t, rows_s):
    parts = []
    for s in (tangent, state):
        s = s.astype(BF16)
        parts += [s[:VL], s[:VL], s[VL:], s[VL:]]
    sums = mm_nt(table, jnp.concatenate(parts, axis=0))
    even = (lane_of(DEV, 2 * DEV) // VL) % 2 == 0
    both = jnp.where(even, sums[:DEV], sums[DEV:])
    rows_t[pl.ds(rho, DEV, stride=RHO), :] = both[:, :DEV]
    rows_s[pl.ds(rho, DEV, stride=RHO), :] = both[:, DEV:]


def write_chunks(send, rows_t, rows_s):
    send[:, 0] = rows_t[...].reshape(DEV, RHO, 128).astype(BF16)
    send[:, 1] = rows_s[...].reshape(DEV, RHO, 128).astype(BF16)


def first_kernel(
    waves, legendre, final, state, send, damped, table, tall, rows_t, rows_s, final_rows, state_rows
):
    damping = damping_row()
    band = lax.axis_index(BAND)
    halve(final, final_rows)
    halve(state.at[0], state_rows)
    degree = lane_of(N, N)
    for rho in range(RHO):
        m = waves[band * RHO + rho]
        kept = jnp.where(degree >= m, legendre[rho].astype(F32), 0.0)
        for h in range(2):
            tall[h] = kept[:, h * 128 : (h + 1) * 128]
        for jj in range(2):
            for h in range(2):
                part = tall[h, pl.ds(jj, DEV, stride=2), :].astype(BF16)
                table[rho, jj * DEV : (jj + 1) * DEV, h * 128 : (h + 1) * 128] = part
        now = damping * strided_rows(final_rows, rho)
        damped[rho] = now
        synth_rho(
            table[rho], now * tangent_scale(m), strided_rows(state_rows, rho), rho, rows_t, rows_s
        )
    write_chunks(send, rows_t, rows_s)


def adjoint_rho(rows, table, rho):
    back = rows[pl.ds(rho, DEV, stride=RHO), :].T
    halves = []
    for p in range(2):
        at = 2 * p * VL
        halves.append(jnp.concatenate([back[at : at + VL], back[at + VL : at + 2 * VL]], axis=1))
    return mm(jnp.concatenate(halves, axis=0).astype(BF16), table)


def turn_kernel(
    step, waves, back, damped_in, table, states, send, damped, rows, rows_t, rows_s, state_rows
):
    damping = damping_row()
    band = lax.axis_index(BAND)
    rows[...] = back[...].astype(F32).reshape(DEV * RHO, 128)
    halve(states.at[step], state_rows)
    for rho in range(RHO):
        now = damping * (damped_in[rho] + adjoint_rho(rows, table[rho], rho))
        damped[rho] = now
        synth_rho(
            table[rho],
            now * tangent_scale(waves[band * RHO + rho]),
            strided_rows(state_rows, rho),
            rho,
            rows_t,
            rows_s,
        )
    write_chunks(send, rows_t, rows_s)


def last_kernel(back, damped_in, table, out, rows, out_rows):
    rows[...] = back[:, 0].astype(F32).reshape(DEV * RHO, 128)
    for rho in range(RHO):
        now = damped_in[rho] + adjoint_rho(rows, table[rho], rho)
        for p in range(2):
            for h in range(2):
                part = now[p * VL : (p + 1) * VL, h * 128 : (h + 1) * 128]
                out_rows[h, pl.ds(p * RHO + rho, VL, stride=2 * RHO), :] = part
    for h in range(2):
        out[:, h * 128 : (h + 1) * 128] = out_rows[h]


def share_kernel(back, bias_part, send):
    total = jnp.sum(back[:, 1].astype(F32), axis=0)
    send[:, 0] = jnp.broadcast_to(total[None], (DEV, 8, 128)).astype(BF16)
    send[:, 1] = jnp.broadcast_to(bias_part[...][None], (DEV, 8, 128)).astype(BF16)


def ending_kernel(parts, w_in_out, w_out_out, bias_out):
    rows = parts[:, 0].astype(F32).reshape(2 * HID, 128)
    w_in_out[...] = rows[:HID].T
    w_out_out[...] = rows[HID:]
    total = jnp.sum(parts[:, 1].astype(F32), axis=0)
    bias_out[...] = total[:4] + total[4:]


def fill_tables(waves, base, w_in, bias, trig, w_in_t, bias_wide):
    m = lax.broadcasted_iota(jnp.int32, (N, N), 0)
    weight = jnp.where(m == 0, 1.0, 2.0).astype(F32)
    pick = jnp.where(m == waves[...], weight, 0.0).T.astype(BF16)
    both = mm(pick, base[...]).astype(BF16)
    trig[:N] = both[:, :LON]
    trig[N:] = both[:, LON:]
    w_in_t[...] = w_in[...].astype(F32).T.astype(BF16)
    bias_wide[...] = jnp.broadcast_to(bias[...], (128, HID)).T


def obs_kernel(obs_time, obs, *outs):
    lev = lax.axis_index("lev")
    for k in range(4):
        to = lax.rem(lev + k, 4)
        for jj in range(2):
            pieces = [obs[i, pl.ds(2 * to + jj, 32, stride=8), :] for i in range(4)]
            for step in range(STEPS):
                total = jnp.zeros((32, 128), F32)
                for i in range(4):
                    total += jnp.where(obs_time[i] == step, 1.0, 0.0).astype(F32) * pieces[i]
                if step == STEPS - 1:
                    outs[k][0, jj] = total.astype(BF16)
                else:
                    outs[4 + k][step, jj] = total.astype(BF16)


def column_kernel(first, last, step, *refs):
    collect = step == STEPS - 2
    refs = list(refs)
    take = lambda count: [refs.pop(0) for _ in range(count)]
    got, w_in, w_out = take(3)
    if first:
        waves, base, bias_row = take(3)
        obs_parts = take(4)
        (send,) = take(1)
        acc, accb, trig, w_in_t, bias = take(5)
        turned, grid, grads, obs, sems = refs
        lev = lax.axis_index("lev")
        copies = [
            pltpu.make_async_copy(obs_parts[k].at[0], obs.at[lax.rem(lev + 4 - k, 4)], sems.at[k])
            for k in range(4)
        ]
        for copy in copies:
            copy.start()
        others = []
        fill_tables(waves, base, w_in, bias_row, trig, w_in_t, bias)
    else:
        trig, w_in_t, bias, acc_in, accb_in = take(5)
        if collect:
            obs_parts = take(4)
            send, acc, accb, obs_all, turned, grid, grads, sems = refs
            lev = lax.axis_index("lev")
            copies, others = [], []
            for k in range(4):
                to = lax.rem(lev + 4 - k, 4)
                copies.append(
                    pltpu.make_async_copy(obs_parts[k].at[step], obs_all.at[step, to], sems.at[k])
                )
                for s in range(step):
                    others.append(
                        pltpu.make_async_copy(
                            obs_parts[k].at[s], obs_all.at[s, to], sems.at[4 * (s + 1) + k]
                        )
                    )
            for copy in copies + others:
                copy.start()
        else:
            copies, others = [], []
            obs_all, send = take(2)
            if last:
                (bias_part,) = take(1)
            acc, accb, turned, grid, grads = refs
        obs = obs_all.at[step]
    for kind in range(2):
        for y in range(4):
            x = got[:, y, kind].reshape(N, 128).T
            for p in range(2):
                for jj in range(2):
                    at = (2 * p + jj) * VL
                    turned[kind, jj, y * VL : (y + 1) * VL, p * N : (p + 1) * N] = x[at : at + VL]
    for kind in range(2):
        for jj in range(2):
            g = mm(turned[kind, jj], trig[...])
            g = jnp.concatenate(
                [g[(y * 4 + v) * 8 : (y * 4 + v + 1) * 8] for v in range(4) for y in range(4)], axis=0
            ).astype(BF16)
            for half in range(2):
                grid[kind, 2 * jj + half] = g[:, half * 256 : (half + 1) * 256]
    if first:
        acc[...] = jnp.zeros_like(acc)
        accb[...] = jnp.zeros_like(accb)
    else:
        acc[...] = acc_in[...]
        accb[...] = accb_in[...]

    for copy in copies:
        copy.wait()

    def block(cb, carry):
        tangent = grid[0, cb]
        features = grid[1, cb]
        back = jnp.zeros((FEAT, 256), F32)
        for hb in range(2):
            rows = slice(hb * 256, (hb + 1) * 256)
            wide = bias[rows, :]
            pre = mm(w_in_t[rows, :], features) + jnp.concatenate([wide, wide], axis=1)
            logistic = 0.5 * jnp.tanh(0.5 * pre) + 0.5
            hidden = (pre * logistic).astype(BF16)
            pre_grad = mm(w_out[rows, :], tangent) * (logistic * (1.0 + pre * (1.0 - logistic)))
            low = pre_grad.astype(BF16)
            acc[rows, :] += mm_nt(low, features)
            acc[hb * 256 + HID : (hb + 1) * 256 + HID, :] += mm_nt(hidden, tangent)
            accb[rows, :] += pre_grad[:, :128] + pre_grad[:, 128:]
            back += mm(w_in[:, rows], low)
        jj = cb // 2
        half = cb % 2
        seen = jnp.concatenate([obs[2 * half + k, jj] for k in range(2)], axis=1)
        back += seen.astype(F32)
        back = jnp.concatenate(
            [back[(v * 4 + y) * 8 : (v * 4 + y + 1) * 8] for y in range(4) for v in range(4)], axis=0
        )
        grads[jj, half] = back.astype(BF16)
        return carry

    lax.fori_loop(0, 4, block, 0, unroll=True)

    real = (lane_of(N, 2 * 128) // 64) % 2 == 0
    for pair in range(2):
        rows = []
        for y in (2 * pair, 2 * pair + 1):
            for _ in range(2):
                for jj in range(2):
                    rows.append(
                        jnp.concatenate(
                            [grads[jj, half, y * VL : (y + 1) * VL, :] for half in range(2)], axis=1
                        )
                    )
        rows = jnp.concatenate(rows, axis=0)
        mixed = jnp.where(real, mm_nt(trig[:N], rows), mm_nt(trig[N:], rows))
        for k in range(2):
            chunk = mixed[:, k * 128 : (k + 1) * 128].reshape(32, 8, 128).astype(BF16)
            if last:
                send[:, 2 * pair + k, 0] = chunk
            else:
                send[:, 2 * pair + k] = chunk
    for copy in others:
        copy.wait()
    if last:
        send[:, :, 1] = acc[...].reshape(32, 4, 8, 128).astype(BF16)
        ones = jnp.ones((8, 128), F32)
        sums = lax.dot_general(
            ones,
            accb[...],
            (((1,), (1,)), ((), ())),
            preferred_element_type=F32,
            precision=lax.Precision.HIGHEST,
        )
        for k in range(4):
            part = sums[:1, k * 128 : (k + 1) * 128]
            high = part.astype(BF16).astype(F32)
            bias_part[k : k + 1, :] = high
            bias_part[k + 4 : k + 5, :] = part - high


VMEM = pl.BlockSpec(memory_space=pltpu.VMEM)
SMEM = pl.BlockSpec(memory_space=pltpu.SMEM)
HBM = pl.BlockSpec(memory_space=pltpu.HBM)


def shape(dims, kind):
    return jax.ShapeDtypeStruct(dims, kind)


def cost(flops, nbytes):
    return pl.CostEstimate(flops=flops, bytes_accessed=nbytes, transcendentals=0)


def whole(dims):
    return pl.BlockSpec(dims, lambda i: (0,) * len(dims))


VMEM_LIMIT = 20 * 1024 * 1024
BIG = 63_000_000
FIRST = 40_000_000


def call(body, ins, outs, scratch, in_specs, flops, nbytes, vmem=VMEM_LIMIT):
    many = isinstance(outs, (list, tuple))
    outs_list = list(outs) if many else [outs]
    out_specs = [whole(o.shape) for o in outs_list]
    return pl.pallas_call(
        body,
        grid=(1,),
        out_shape=outs_list if many else outs,
        in_specs=in_specs,
        out_specs=out_specs if many else out_specs[0],
        scratch_shapes=scratch,
        cost_estimate=cost(flops, nbytes),
        compiler_params=pltpu.CompilerParams(vmem_limit_bytes=vmem),
    )(*ins)


def exchange(array, axes):
    return lax.all_to_all(array, axes, split_axis=0, concat_axis=0, tiled=True)


def trig_base():
    phase = (np.arange(N)[:, None] * np.arange(LON)[None, :]) % LON
    angle = 2.0 * np.pi / LON * phase
    return jnp.asarray(np.concatenate([np.cos(angle), -np.sin(angle)], axis=1), BF16)


def program(checkpoints, final_cot, obs_cot, obs_time, wave_order, legendre, w_in, w_out, bias):
    states = checkpoints.reshape(STEPS, 512, N)
    final = final_cot.reshape(512, N)
    seen = obs_cot.reshape(4, FEAT * 8, 128)
    state_spec = pl.BlockSpec((1, 512, N), lambda i: (STEPS - 1, 0, 0))
    chunks = shape((DEV, 2, RHO, 128), BF16)
    tall = pltpu.VMEM((DEV * RHO, 128), F32)
    halves = pltpu.VMEM((2, 512, 128), F32)

    send, damped, table = call(
        first_kernel,
        (wave_order, legendre, final, states),
        (chunks, shape((RHO, 64, N), F32), shape((RHO, N, N), BF16)),
        [
            pltpu.VMEM((2, N, 128), F32),
            tall,
            tall,
            halves,
            halves,
        ],
        [SMEM, whole(legendre.shape), whole(final.shape), state_spec],
        300_000_000,
        4_000_000,
        BIG,
    )
    obs_shapes = [(1, 2, FEAT, 128)] * 4 + [(STEPS - 1, 2, FEAT, 128)] * 4
    obs_parts = pl.pallas_call(
        obs_kernel,
        grid=(4,),
        out_shape=[shape(d, BF16) for d in obs_shapes],
        in_specs=[SMEM, pl.BlockSpec((4, 256, 128), lambda g: (0, g, 0))],
        out_specs=[pl.BlockSpec(d[:2] + (32, 128), lambda g: (0, 0, g, 0)) for d in obs_shapes],
        cost_estimate=cost(10_000_000, 3_000_000),
        compiler_params=pltpu.CompilerParams(vmem_limit_bytes=BIG),
        name="obs",
    )(obs_time, seen)
    obs_cols = []
    for k, part in enumerate(obs_parts):
        if k % 4:
            part = lax.ppermute(part, "lev", [(i, (i + k) % 4) for i in range(4)])
        obs_cols.append(part)

    sums = ()
    for step in reversed(range(STEPS)):
        first = step == STEPS - 1
        last = step == 0
        got = exchange(send, ALL).reshape(32, 4, 2, RHO, 128)
        acc_shapes = [shape((2 * HID, 128), F32), shape((HID, 128), F32)]
        scratch = [
            pltpu.VMEM((2, 2, FEAT, 2 * N), BF16),
            pltpu.VMEM((2, 4, FEAT, 256), BF16),
            pltpu.VMEM((2, 2, FEAT, 256), BF16),
        ]
        outs = [shape((32, 4, RHO, 128), BF16)] + acc_shapes
        ins = [got, w_in, w_out]
        if first:
            ins += [wave_order.reshape(1, N), trig_base(), bias.reshape(1, HID)]
            outs += [shape((2 * N, LON), BF16), shape((HID, FEAT), BF16), shape((HID, 128), F32)]
            scratch += [pltpu.VMEM((4, 2, FEAT, 128), BF16), pltpu.SemaphoreType.DMA((4,))]
            specs = [whole(a.shape) for a in ins] + [HBM] * 4
            ins += obs_cols[:4]
        else:
            ins += [trig, w_in_t, bias_wide, *sums]
            specs = [whole(a.shape) for a in ins]
            if step == STEPS - 2:
                ins += obs_cols[4:]
                specs += [HBM] * 4
                outs.append(shape((STEPS - 1, 4, 2, FEAT, 128), BF16))
                scratch.append(pltpu.SemaphoreType.DMA((4 * (STEPS - 1),)))
            else:
                ins.append(obs_all)
                specs.append(whole(obs_all.shape))
        if last:
            outs = [shape((32, 4, 2, RHO, 128), BF16), shape((8, 128), F32)]
            scratch = [pltpu.VMEM(a.shape, F32) for a in acc_shapes] + scratch
        back, *sums = call(
            functools.partial(column_kernel, first, last, step),
            ins,
            outs,
            scratch,
            specs,
            1_200_000_000,
            3_000_000,
            FIRST if first else VMEM_LIMIT,
        )
        if first:
            trig, w_in_t, bias_wide = sums[2:]
            sums = sums[:2]
        elif not last and len(sums) > 2:
            obs_all = sums.pop()
        if not last:
            back = exchange(back.reshape(DEV, RHO, 128), ALL)
            ins = [wave_order, back, damped, table, states]
            specs = [SMEM, whole(back.shape), whole(damped.shape), whole(table.shape), whole(states.shape)]
            outs = [chunks, shape((RHO, 64, N), F32)]
            scratch = [tall, tall, tall, halves]
            send, damped = call(
                functools.partial(turn_kernel, step - 1),
                ins,
                outs,
                scratch,
                specs,
                400_000_000,
                4_000_000,
            )
    back = exchange(back.reshape(DEV, 2, RHO, 128), ALL)
    (bias_part,) = sums
    parts = call(
        share_kernel,
        (back, bias_part),
        chunks,
        [],
        [whole(back.shape), whole(bias_part.shape)],
        1_000_000,
        1_000_000,
    )
    parts = exchange(parts, ALL)
    adjoint = call(
        last_kernel,
        (back, damped, table),
        shape((512, N), F32),
        [tall, halves],
        [whole(back.shape), whole(damped.shape), whole(table.shape)],
        100_000_000,
        3_000_000,
    )
    grad_w_in, grad_w_out, grad_bias = call(
        ending_kernel,
        (parts,),
        (shape((FEAT, HID), F32), shape((HID, FEAT), F32), shape((4, 128), F32)),
        [],
        [whole(parts.shape)],
        1_000_000,
        1_500_000,
    )
    return (adjoint.reshape(final_cot.shape), grad_w_in, grad_w_out, grad_bias.reshape(HID))


def solution(mesh):
    torus = Mesh(mesh.devices.reshape(4, 4, 2, mesh.shape["lev"]), ("band_0", "band_1", "band_2", "lev"))
    placed = (
        P(None, None, "lev", None, BAND, None),
        P(None, "lev", None, BAND, None),
        P(None, None, None, BAND, "lev"),
        P(),
        P(),
        P(BAND, None, None),
        P(),
        P(),
        P(),
    )
    return jax.shard_map(
        program,
        mesh=torus,
        in_specs=placed,
        out_specs=(P(None, "lev", None, BAND, None), P(), P(), P()),
        check_vma=False,
    )
```

```python
import functools

import jax
import jax.numpy as jnp
import numpy as np
from jax import lax
from jax.experimental import pallas as pl
from jax.experimental.pallas import tpu as pltpu
from jax.sharding import Mesh
from jax.sharding import PartitionSpec as P

BAND = ("band_0", "band_1", "band_2")
ALL = ("band_0", "band_1", "band_2", "lev")
F32 = jnp.float32
BF16 = jnp.bfloat16

RHO = 8
N = 256
LON = 512
FEAT = 128
HID = 512
STEPS = 4
VL = 32
DEV = 128


def mm(a, b):
    return jnp.dot(a, b, preferred_element_type=F32)


def mm_nt(a, b):
    return lax.dot_general(a, b, (((1,), (1,)), ((), ())), preferred_element_type=F32)


def lane_of(rows, lanes):
    return lax.broadcasted_iota(jnp.int32, (rows, lanes), 1)


def damping_row():
    n = lane_of(1, N).astype(F32)
    return 1.0 / (1.0 + 2.0 * n * (n + 1.0) / (N * N))


def halve(ref, halves):
    for h in range(2):
        halves[h] = ref[:, h * 128 : (h + 1) * 128]


def strided_rows(halves, rho):
    return jnp.concatenate(
        [
            jnp.concatenate(
                [halves[h, pl.ds(p * RHO + rho, VL, stride=2 * RHO), :] for h in range(2)], axis=1
            )
            for p in range(2)
        ],
        axis=0,
    )


def tangent_scale(m):
    return jnp.where(m == 0, 1.0 / LON, 0.5 / LON).astype(F32)


def synth_rho(table, tangent, state, rho, rows_t, rows_s):
    parts = []
    for s in (tangent, state):
        s = s.astype(BF16)
        parts += [s[:VL], s[:VL], s[VL:], s[VL:]]
    sums = mm_nt(table, jnp.concatenate(parts, axis=0))
    even = (lane_of(DEV, 2 * DEV) // VL) % 2 == 0
    both = jnp.where(even, sums[:DEV], sums[DEV:])
    rows_t[pl.ds(rho, DEV, stride=RHO), :] = both[:, :DEV]
    rows_s[pl.ds(rho, DEV, stride=RHO), :] = both[:, DEV:]


def write_chunks(send, rows_t, rows_s):
    send[:, 0] = rows_t[...].reshape(DEV, RHO, 128).astype(BF16)
    send[:, 1] = rows_s[...].reshape(DEV, RHO, 128).astype(BF16)


def first_kernel(
    waves, legendre, final, state, send, damped, table, tall, rows_t, rows_s, final_rows, state_rows
):
    damping = damping_row()
    band = lax.axis_index(BAND)
    halve(final, final_rows)
    halve(state.at[0], state_rows)
    degree = lane_of(N, N)
    for rho in range(RHO):
        m = waves[band * RHO + rho]
        kept = jnp.where(degree >= m, legendre[rho].astype(F32), 0.0)
        for h in range(2):
            tall[h] = kept[:, h * 128 : (h + 1) * 128]
        for jj in range(2):
            for h in range(2):
                part = tall[h, pl.ds(jj, DEV, stride=2), :].astype(BF16)
                table[rho, jj * DEV : (jj + 1) * DEV, h * 128 : (h + 1) * 128] = part
        now = damping * strided_rows(final_rows, rho)
        damped[rho] = now
        synth_rho(
            table[rho], now * tangent_scale(m), strided_rows(state_rows, rho), rho, rows_t, rows_s
        )
    write_chunks(send, rows_t, rows_s)


def adjoint_rho(rows, table, rho):
    back = rows[pl.ds(rho, DEV, stride=RHO), :].astype(BF16).T
    halves = []
    for p in range(2):
        at = 2 * p * VL
        halves.append(jnp.concatenate([back[at : at + VL], back[at + VL : at + 2 * VL]], axis=1))
    return mm(jnp.concatenate(halves, axis=0), table)


def turn_kernel(
    step, waves, back, damped_in, table, states, send, damped, rows, rows_t, rows_s, state_rows
):
    damping = damping_row()
    band = lax.axis_index(BAND)
    rows[...] = back[...].astype(F32).reshape(DEV * RHO, 128)
    halve(states.at[step], state_rows)
    for rho in range(RHO):
        now = damping * (damped_in[rho] + adjoint_rho(rows, table[rho], rho))
        damped[rho] = now
        synth_rho(
            table[rho],
            now * tangent_scale(waves[band * RHO + rho]),
            strided_rows(state_rows, rho),
            rho,
            rows_t,
            rows_s,
        )
    write_chunks(send, rows_t, rows_s)


def last_kernel(back, damped_in, table, out, rows, out_rows):
    rows[...] = back[:, 0].astype(F32).reshape(DEV * RHO, 128)
    for rho in range(RHO):
        now = damped_in[rho] + adjoint_rho(rows, table[rho], rho)
        for p in range(2):
            for h in range(2):
                part = now[p * VL : (p + 1) * VL, h * 128 : (h + 1) * 128]
                out_rows[h, pl.ds(p * RHO + rho, VL, stride=2 * RHO), :] = part
    for h in range(2):
        out[:, h * 128 : (h + 1) * 128] = out_rows[h]


def share_kernel(back, bias_part, send):
    total = jnp.sum(back[:, 1].astype(F32), axis=0)
    for part, rows in enumerate((total[:4], total[4:], bias_part[...])):
        send[:, part] = jnp.broadcast_to(rows[None], (DEV, 4, 128)).astype(BF16)


def ending_kernel(parts, w_in_out, w_out_out, bias_out, rows):
    for d in range(DEV):
        for half in range(2):
            rows[8 * d + 4 * half : 8 * d + 4 * half + 4, :] = parts[d, half].astype(F32)
    w_in_out[...] = rows[:HID].T
    w_out_out[...] = rows[HID:]
    bias_out[...] = jnp.sum(parts[:, 2].astype(F32), axis=0)


def fill_tables(waves, base, w_in, bias, trig, w_in_t, bias_wide):
    m = lax.broadcasted_iota(jnp.int32, (N, N), 0)
    weight = jnp.where(m == 0, 1.0, 2.0).astype(F32)
    pick = jnp.where(m == waves[...], weight, 0.0).T.astype(BF16)
    both = mm(pick, base[...]).astype(BF16)
    trig[:N] = both[:, :LON]
    trig[N:] = both[:, LON:]
    w_in_t[...] = w_in[...].astype(F32).T.astype(BF16)
    bias_wide[...] = jnp.broadcast_to(bias[...], (128, HID)).T


def obs_kernel(obs_time, obs, *outs):
    lev = lax.axis_index("lev")
    for k in range(4):
        to = lax.rem(lev + k, 4)
        for jj in range(2):
            pieces = [obs[i, pl.ds(2 * to + jj, 64, stride=8), :] for i in range(4)]
            for step in range(STEPS):
                total = jnp.zeros((64, 128), F32)
                for i in range(4):
                    total += jnp.where(obs_time[i] == step, 1.0, 0.0).astype(F32) * pieces[i]
                if step == STEPS - 1:
                    outs[k][0, jj] = total.astype(BF16)
                else:
                    outs[4 + k][step, jj] = total.astype(BF16)


def column_kernel(first, last, step, *refs):
    collect = step == STEPS - 2
    refs = list(refs)
    take = lambda count: [refs.pop(0) for _ in range(count)]
    got, w_in, w_out = take(3)
    if first:
        waves, base, bias_row = take(3)
        obs_parts = take(4)
        (send,) = take(1)
        acc, accb, trig, w_in_t, bias = take(5)
        turned, grid, grads, obs = refs
        lev = lax.axis_index("lev")
        for k in range(4):
            obs[lax.rem(lev + 4 - k, 4)] = obs_parts[k][0]
        fill_tables(waves, base, w_in, bias_row, trig, w_in_t, bias)
    else:
        trig, w_in_t, bias, acc_in, accb_in = take(5)
        if collect:
            obs_parts = take(4)
            send, acc, accb, obs_all, turned, grid, grads = refs
            lev = lax.axis_index("lev")
            for k in range(4):
                for s in range(STEPS - 1):
                    obs_all[s, lax.rem(lev + 4 - k, 4)] = obs_parts[k][s]
        else:
            obs_all, send = take(2)
            if last:
                (bias_part,) = take(1)
            acc, accb, turned, grid, grads = refs
        obs = obs_all.at[step]
    for kind in range(2):
        for y in range(4):
            x = got[:, y, kind].reshape(N, 128).T
            for p in range(2):
                for jj in range(2):
                    at = (2 * p + jj) * VL
                    turned[kind, jj, y * VL : (y + 1) * VL, p * N : (p + 1) * N] = x[at : at + VL]
    for kind in range(2):
        for jj in range(2):
            g = mm(turned[kind, jj], trig[...])
            g = jnp.concatenate(
                [g[(y * 4 + v) * 8 : (y * 4 + v + 1) * 8] for v in range(4) for y in range(4)], axis=0
            ).astype(BF16)
            for half in range(2):
                grid[kind, 2 * jj + half] = g[:, half * 256 : (half + 1) * 256]
    if first:
        acc[...] = jnp.zeros_like(acc)
        accb[...] = jnp.zeros_like(accb)
    else:
        acc[...] = acc_in[...]
        accb[...] = accb_in[...]

    def block(cb, carry):
        tangent = grid[0, cb]
        features = grid[1, cb]
        back = jnp.zeros((FEAT, 256), F32)
        for hb in range(2):
            rows = slice(hb * 256, (hb + 1) * 256)
            wide = bias[rows, :]
            pre = mm(w_in_t[rows, :], features) + jnp.concatenate([wide, wide], axis=1)
            logistic = 0.5 * jnp.tanh(0.5 * pre) + 0.5
            hidden = (pre * logistic).astype(BF16)
            pre_grad = mm(w_out[rows, :], tangent) * (logistic * (1.0 + pre * (1.0 - logistic)))
            low = pre_grad.astype(BF16)
            acc[rows, :] += mm_nt(low, features)
            acc[hb * 256 + HID : (hb + 1) * 256 + HID, :] += mm_nt(hidden, tangent)
            accb[rows, :] += pre_grad[:, :128] + pre_grad[:, 128:]
            back += mm(w_in[:, rows], low)
        jj = cb // 2
        half = cb % 2
        seen = jnp.concatenate([obs[2 * half + k, jj] for k in range(2)], axis=1)
        back += seen.astype(F32)
        back = jnp.concatenate(
            [back[(v * 4 + y) * 8 : (v * 4 + y + 1) * 8] for y in range(4) for v in range(4)], axis=0
        )
        grads[jj, half] = back.astype(BF16)
        return carry

    lax.fori_loop(0, 4, block, 0, unroll=True)

    real = (lane_of(N, 2 * 128) // 64) % 2 == 0
    for pair in range(2):
        rows = []
        for y in (2 * pair, 2 * pair + 1):
            for _ in range(2):
                for jj in range(2):
                    rows.append(
                        jnp.concatenate(
                            [grads[jj, half, y * VL : (y + 1) * VL, :] for half in range(2)], axis=1
                        )
                    )
        rows = jnp.concatenate(rows, axis=0)
        mixed = jnp.where(real, mm_nt(trig[:N], rows), mm_nt(trig[N:], rows))
        for k in range(2):
            chunk = mixed[:, k * 128 : (k + 1) * 128].reshape(32, 8, 128).astype(BF16)
            if last:
                send[:, 2 * pair + k, 0] = chunk
            else:
                send[:, 2 * pair + k] = chunk
    if last:
        send[:, :, 1] = acc[...].reshape(32, 4, 8, 128).astype(BF16)
        ones = jnp.ones((8, 128), F32)
        sums = lax.dot_general(
            ones,
            accb[...],
            (((1,), (1,)), ((), ())),
            preferred_element_type=F32,
            precision=lax.Precision.HIGHEST,
        )
        for k in range(4):
            bias_part[k : k + 1, :] = sums[:1, k * 128 : (k + 1) * 128]


VMEM = pl.BlockSpec(memory_space=pltpu.VMEM)
SMEM = pl.BlockSpec(memory_space=pltpu.SMEM)
HBM = pl.BlockSpec(memory_space=pltpu.HBM)


def shape(dims, kind):
    return jax.ShapeDtypeStruct(dims, kind)


def cost(flops, nbytes):
    return pl.CostEstimate(flops=flops, bytes_accessed=nbytes, transcendentals=0)


def whole(dims):
    return pl.BlockSpec(dims, lambda i: (0,) * len(dims))


VMEM_LIMIT = 20 * 1024 * 1024
BIG = 63_000_000
FIRST = 40_000_000


def call(body, ins, outs, scratch, in_specs, flops, nbytes, vmem=VMEM_LIMIT):
    many = isinstance(outs, (list, tuple))
    outs_list = list(outs) if many else [outs]
    out_specs = [whole(o.shape) for o in outs_list]
    return pl.pallas_call(
        body,
        grid=(1,),
        out_shape=outs_list if many else outs,
        in_specs=in_specs,
        out_specs=out_specs if many else out_specs[0],
        scratch_shapes=scratch,
        cost_estimate=cost(flops, nbytes),
        compiler_params=pltpu.CompilerParams(vmem_limit_bytes=vmem),
    )(*ins)


def exchange(array, axes):
    return lax.all_to_all(array, axes, split_axis=0, concat_axis=0, tiled=True)


def trig_base():
    phase = (np.arange(N)[:, None] * np.arange(LON)[None, :]) % LON
    angle = 2.0 * np.pi / LON * phase
    return jnp.asarray(np.concatenate([np.cos(angle), -np.sin(angle)], axis=1), BF16)


def program(checkpoints, final_cot, obs_cot, obs_time, wave_order, legendre, w_in, w_out, bias):
    states = checkpoints.reshape(STEPS, 512, N)
    final = final_cot.reshape(512, N)
    seen = obs_cot.reshape(4, FEAT * 8, 128)
    state_spec = pl.BlockSpec((1, 512, N), lambda i: (STEPS - 1, 0, 0))
    chunks = shape((DEV, 2, RHO, 128), BF16)
    tall = pltpu.VMEM((DEV * RHO, 128), F32)
    halves = pltpu.VMEM((2, 512, 128), F32)

    send, damped, table = call(
        first_kernel,
        (wave_order, legendre, final, states),
        (chunks, shape((RHO, 64, N), F32), shape((RHO, N, N), BF16)),
        [
            pltpu.VMEM((2, N, 128), F32),
            tall,
            tall,
            halves,
            halves,
        ],
        [SMEM, whole(legendre.shape), whole(final.shape), state_spec],
        300_000_000,
        4_000_000,
        BIG,
    )
    obs_shapes = [(1, 2, FEAT, 128)] * 4 + [(STEPS - 1, 2, FEAT, 128)] * 4
    obs_parts = pl.pallas_call(
        obs_kernel,
        grid=(2,),
        out_shape=[shape(d, BF16) for d in obs_shapes],
        in_specs=[SMEM, pl.BlockSpec((4, 512, 128), lambda g: (0, g, 0))],
        out_specs=[pl.BlockSpec(d[:2] + (64, 128), lambda g: (0, 0, g, 0)) for d in obs_shapes],
        cost_estimate=cost(10_000_000, 3_000_000),
        compiler_params=pltpu.CompilerParams(vmem_limit_bytes=BIG),
        name="obs",
    )(obs_time, seen)
    obs_cols = []
    for k, part in enumerate(obs_parts):
        if k % 4:
            part = lax.ppermute(part, "lev", [(i, (i + k) % 4) for i in range(4)])
        obs_cols.append(part)

    sums = ()
    for step in reversed(range(STEPS)):
        first = step == STEPS - 1
        last = step == 0
        got = exchange(send, ALL).reshape(32, 4, 2, RHO, 128)
        acc_shapes = [shape((2 * HID, 128), F32), shape((HID, 128), F32)]
        scratch = [
            pltpu.VMEM((2, 2, FEAT, 2 * N), BF16),
            pltpu.VMEM((2, 4, FEAT, 256), BF16),
            pltpu.VMEM((2, 2, FEAT, 256), BF16),
        ]
        outs = [shape((32, 4, RHO, 128), BF16)] + acc_shapes
        ins = [got, w_in, w_out]
        if first:
            ins += [wave_order.reshape(1, N), trig_base(), bias.reshape(1, HID)]
            outs += [shape((2 * N, LON), BF16), shape((HID, FEAT), BF16), shape((HID, 128), F32)]
            scratch += [pltpu.VMEM((4, 2, FEAT, 128), BF16)]
            ins += obs_cols[:4]
            specs = [whole(a.shape) for a in ins]
        else:
            ins += [trig, w_in_t, bias_wide, *sums]
            specs = [whole(a.shape) for a in ins]
            if step == STEPS - 2:
                ins += obs_cols[4:]
                specs = [whole(a.shape) for a in ins]
                outs.append(shape((STEPS - 1, 4, 2, FEAT, 128), BF16))
            else:
                ins.append(obs_all)
                specs.append(whole(obs_all.shape))
        if last:
            outs = [shape((32, 4, 2, RHO, 128), BF16), shape((4, 128), F32)]
            scratch = [pltpu.VMEM(a.shape, F32) for a in acc_shapes] + scratch
        back, *sums = call(
            functools.partial(column_kernel, first, last, step),
            ins,
            outs,
            scratch,
            specs,
            1_200_000_000,
            3_000_000,
            FIRST if first else VMEM_LIMIT,
        )
        if first:
            trig, w_in_t, bias_wide = sums[2:]
            sums = sums[:2]
        elif not last and len(sums) > 2:
            obs_all = sums.pop()
        if not last:
            back = exchange(back.reshape(DEV, RHO, 128), ALL)
            ins = [wave_order, back, damped, table, states]
            specs = [SMEM, whole(back.shape), whole(damped.shape), whole(table.shape), whole(states.shape)]
            outs = [chunks, shape((RHO, 64, N), F32)]
            scratch = [tall, tall, tall, halves]
            send, damped = call(
                functools.partial(turn_kernel, step - 1),
                ins,
                outs,
                scratch,
                specs,
                400_000_000,
                4_000_000,
            )
    back = exchange(back.reshape(DEV, 2, RHO, 128), ALL)
    (bias_part,) = sums
    parts = call(
        share_kernel,
        (back, bias_part),
        shape((DEV, 3, 4, 128), BF16),
        [],
        [whole(back.shape), whole(bias_part.shape)],
        1_000_000,
        1_000_000,
    )
    parts = exchange(parts, ALL)
    adjoint = call(
        last_kernel,
        (back, damped, table),
        shape((512, N), F32),
        [tall, halves],
        [whole(back.shape), whole(damped.shape), whole(table.shape)],
        100_000_000,
        3_000_000,
    )
    grad_w_in, grad_w_out, grad_bias = call(
        ending_kernel,
        (parts,),
        (shape((FEAT, HID), F32), shape((HID, FEAT), F32), shape((4, 128), F32)),
        [tall],
        [whole(parts.shape)],
        1_000_000,
        1_500_000,
    )
    return (adjoint.reshape(final_cot.shape), grad_w_in, grad_w_out, grad_bias.reshape(HID))


def solution(mesh):
    torus = Mesh(mesh.devices.reshape(4, 4, 2, mesh.shape["lev"]), ("band_0", "band_1", "band_2", "lev"))
    placed = (
        P(None, None, "lev", None, BAND, None),
        P(None, "lev", None, BAND, None),
        P(None, None, None, BAND, "lev"),
        P(),
        P(),
        P(BAND, None, None),
        P(),
        P(),
        P(),
    )
    return jax.shard_map(
        program,
        mesh=torus,
        in_specs=placed,
        out_specs=(P(None, "lev", None, BAND, None), P(), P(), P()),
        check_vma=False,
    )
```

```python
import functools

import jax
import jax.numpy as jnp
import numpy as np
from jax import lax
from jax.experimental import pallas as pl
from jax.experimental.pallas import tpu as pltpu
from jax.sharding import Mesh
from jax.sharding import PartitionSpec as P

BAND = ("band_0", "band_1", "band_2")
ALL = ("band_0", "band_1", "band_2", "lev")
F32 = jnp.float32
BF16 = jnp.bfloat16

RHO = 8
N = 256
LON = 512
FEAT = 128
HID = 512
STEPS = 4
VL = 32
DEV = 128


def mm(a, b):
    return jnp.dot(a, b, preferred_element_type=F32)


def mm_nt(a, b):
    return lax.dot_general(a, b, (((1,), (1,)), ((), ())), preferred_element_type=F32)


def lane_of(rows, lanes):
    return lax.broadcasted_iota(jnp.int32, (rows, lanes), 1)


def damping_row():
    n = lane_of(1, N).astype(F32)
    return 1.0 / (1.0 + 2.0 * n * (n + 1.0) / (N * N))


def halve(ref, halves):
    for h in range(2):
        halves[h] = ref[:, h * 128 : (h + 1) * 128]


def strided_rows(halves, rho):
    return jnp.concatenate(
        [
            jnp.concatenate(
                [halves[h, pl.ds(p * RHO + rho, VL, stride=2 * RHO), :] for h in range(2)], axis=1
            )
            for p in range(2)
        ],
        axis=0,
    )


def tangent_scale(m):
    return jnp.where(m == 0, 1.0 / LON, 0.5 / LON).astype(F32)


def synth_rho(table, tangent, state, rho, rows_t, rows_s):
    parts = []
    for s in (tangent, state):
        s = s.astype(BF16)
        parts += [s[:VL], s[:VL], s[VL:], s[VL:]]
    sums = mm_nt(table, jnp.concatenate(parts, axis=0))
    even = (lane_of(DEV, 2 * DEV) // VL) % 2 == 0
    both = jnp.where(even, sums[:DEV], sums[DEV:])
    rows_t[pl.ds(rho, DEV, stride=RHO), :] = both[:, :DEV]
    rows_s[pl.ds(rho, DEV, stride=RHO), :] = both[:, DEV:]


def write_chunks(send, rows_t, rows_s):
    send[:, 0] = rows_t[...].reshape(DEV, RHO, 128).astype(BF16)
    send[:, 1] = rows_s[...].reshape(DEV, RHO, 128).astype(BF16)


def first_kernel(
    waves, legendre, final, state, send, damped, table, tall, rows_t, rows_s, final_rows, state_rows
):
    damping = damping_row()
    band = lax.axis_index(BAND)
    halve(final, final_rows)
    halve(state.at[0], state_rows)
    degree = lane_of(N, N)
    for rho in range(RHO):
        m = waves[band * RHO + rho]
        kept = jnp.where(degree >= m, legendre[rho].astype(F32), 0.0)
        for h in range(2):
            tall[h] = kept[:, h * 128 : (h + 1) * 128]
        for jj in range(2):
            for h in range(2):
                part = tall[h, pl.ds(jj, DEV, stride=2), :].astype(BF16)
                table[rho, jj * DEV : (jj + 1) * DEV, h * 128 : (h + 1) * 128] = part
        now = damping * strided_rows(final_rows, rho)
        damped[rho] = now
        synth_rho(
            table[rho], now * tangent_scale(m), strided_rows(state_rows, rho), rho, rows_t, rows_s
        )
    write_chunks(send, rows_t, rows_s)


def adjoint_rho(rows, table, rho):
    back = rows[pl.ds(rho, DEV, stride=RHO), :].astype(BF16).T
    halves = []
    for p in range(2):
        at = 2 * p * VL
        halves.append(jnp.concatenate([back[at : at + VL], back[at + VL : at + 2 * VL]], axis=1))
    return mm(jnp.concatenate(halves, axis=0), table)


def turn_kernel(
    step, waves, back, damped_in, table, states, send, damped, rows, rows_t, rows_s, state_rows
):
    damping = damping_row()
    band = lax.axis_index(BAND)
    rows[...] = back[...].astype(F32).reshape(DEV * RHO, 128)
    halve(states.at[step], state_rows)
    for rho in range(RHO):
        now = damping * (damped_in[rho] + adjoint_rho(rows, table[rho], rho))
        damped[rho] = now
        synth_rho(
            table[rho],
            now * tangent_scale(waves[band * RHO + rho]),
            strided_rows(state_rows, rho),
            rho,
            rows_t,
            rows_s,
        )
    write_chunks(send, rows_t, rows_s)


def last_kernel(back, damped_in, table, out, rows, out_rows):
    rows[...] = back[:, 0].astype(F32).reshape(DEV * RHO, 128)
    for rho in range(RHO):
        now = damped_in[rho] + adjoint_rho(rows, table[rho], rho)
        for p in range(2):
            for h in range(2):
                part = now[p * VL : (p + 1) * VL, h * 128 : (h + 1) * 128]
                out_rows[h, pl.ds(p * RHO + rho, VL, stride=2 * RHO), :] = part
    for h in range(2):
        out[:, h * 128 : (h + 1) * 128] = out_rows[h]


def share_kernel(back, bias_part, send):
    total = jnp.sum(back[:, 1].astype(F32), axis=0)
    for part, rows in enumerate((total[:4], total[4:], bias_part[...])):
        send[:, part] = jnp.broadcast_to(rows[None], (DEV, 4, 128)).astype(BF16)


def ending_kernel(parts, w_in_out, w_out_out, bias_out, rows):
    for d in range(DEV):
        for half in range(2):
            rows[8 * d + 4 * half : 8 * d + 4 * half + 4, :] = parts[d, half].astype(F32)
    w_in_out[...] = rows[:HID].T
    w_out_out[...] = rows[HID:]
    bias_out[...] = jnp.sum(parts[:, 2].astype(F32), axis=0)


def fill_tables(waves, base, w_in, bias, trig, w_in_t, bias_wide):
    m = lax.broadcasted_iota(jnp.int32, (N, N), 0)
    weight = jnp.where(m == 0, 1.0, 2.0).astype(F32)
    pick = jnp.where(m == waves[...], weight, 0.0).T.astype(BF16)
    both = mm(pick, base[...]).astype(BF16)
    trig[:N] = both[:, :LON]
    trig[N:] = both[:, LON:]
    w_in_t[...] = w_in[...].astype(F32).T.astype(BF16)
    bias_wide[...] = jnp.broadcast_to(bias[...], (128, HID)).T


def obs_kernel(obs_time, obs, *outs):
    lev = lax.axis_index("lev")
    for k in range(4):
        to = lax.rem(lev + k, 4)
        for jj in range(2):
            pieces = [obs[i, pl.ds(2 * to + jj, 64, stride=8), :] for i in range(4)]
            for step in range(STEPS):
                total = jnp.zeros((64, 128), F32)
                for i in range(4):
                    total += jnp.where(obs_time[i] == step, 1.0, 0.0).astype(F32) * pieces[i]
                if step == STEPS - 1:
                    outs[k][0, jj] = total.astype(BF16)
                else:
                    outs[4 + k][step, jj] = total.astype(BF16)


def column_kernel(first, last, step, *refs):
    collect = step == STEPS - 2
    refs = list(refs)
    take = lambda count: [refs.pop(0) for _ in range(count)]
    got, w_in, w_out = take(3)
    if first:
        waves, base, bias_row = take(3)
        obs_parts = take(4)
        (send,) = take(1)
        acc, accb, trig, w_in_t, bias = take(5)
        turned, grid, grads, obs = refs
        lev = lax.axis_index("lev")
        for k in range(4):
            obs[lax.rem(lev + 4 - k, 4)] = obs_parts[k][0]
        fill_tables(waves, base, w_in, bias_row, trig, w_in_t, bias)
    else:
        trig, w_in_t, bias, acc_in, accb_in = take(5)
        if collect:
            obs_parts = take(4)
            send, acc, accb, obs_all, turned, grid, grads = refs
            lev = lax.axis_index("lev")
            for k in range(4):
                for s in range(STEPS - 1):
                    obs_all[s, lax.rem(lev + 4 - k, 4)] = obs_parts[k][s]
        else:
            obs_all, send = take(2)
            if last:
                (bias_part,) = take(1)
            acc, accb, turned, grid, grads = refs
        obs = obs_all.at[step]
    for kind in range(2):
        for y in range(4):
            x = got[:, y, kind].reshape(N, 128).T
            for p in range(2):
                for jj in range(2):
                    at = (2 * p + jj) * VL
                    turned[kind, jj, y * VL : (y + 1) * VL, p * N : (p + 1) * N] = x[at : at + VL]
    for kind in range(2):
        for jj in range(2):
            g = mm(turned[kind, jj], trig[...])
            g = jnp.concatenate(
                [g[(y * 4 + v) * 8 : (y * 4 + v + 1) * 8] for v in range(4) for y in range(4)], axis=0
            ).astype(BF16)
            for half in range(2):
                grid[kind, 2 * jj + half] = g[:, half * 256 : (half + 1) * 256]
    if first:
        acc[...] = jnp.zeros_like(acc)
        accb[...] = jnp.zeros_like(accb)
    else:
        acc[...] = acc_in[...]
        accb[...] = accb_in[...]

    def block(cb, carry):
        tangent = grid[0, cb]
        features = grid[1, cb]
        back = jnp.zeros((FEAT, 256), F32)
        for hb in range(1):
            rows = slice(hb * 512, (hb + 1) * 512)
            wide = bias[rows, :]
            pre = mm(w_in_t[rows, :], features) + jnp.concatenate([wide, wide], axis=1)
            logistic = 0.5 * jnp.tanh(0.5 * pre) + 0.5
            hidden = (pre * logistic).astype(BF16)
            pre_grad = mm(w_out[rows, :], tangent) * (logistic * (1.0 + pre * (1.0 - logistic)))
            low = pre_grad.astype(BF16)
            acc[rows, :] += mm_nt(low, features)
            acc[hb * 512 + HID : (hb + 1) * 512 + HID, :] += mm_nt(hidden, tangent)
            accb[rows, :] += pre_grad[:, :128] + pre_grad[:, 128:]
            back += mm(w_in[:, rows], low)
        jj = cb // 2
        half = cb % 2
        seen = jnp.concatenate([obs[2 * half + k, jj] for k in range(2)], axis=1)
        back += seen.astype(F32)
        back = jnp.concatenate(
            [back[(v * 4 + y) * 8 : (v * 4 + y + 1) * 8] for y in range(4) for v in range(4)], axis=0
        )
        grads[jj, half] = back.astype(BF16)
        return carry

    lax.fori_loop(0, 4, block, 0, unroll=True)

    real = (lane_of(N, 2 * 128) // 64) % 2 == 0
    for pair in range(2):
        rows = []
        for y in (2 * pair, 2 * pair + 1):
            for _ in range(2):
                for jj in range(2):
                    rows.append(
                        jnp.concatenate(
                            [grads[jj, half, y * VL : (y + 1) * VL, :] for half in range(2)], axis=1
                        )
                    )
        rows = jnp.concatenate(rows, axis=0)
        mixed = jnp.where(real, mm_nt(trig[:N], rows), mm_nt(trig[N:], rows))
        for k in range(2):
            chunk = mixed[:, k * 128 : (k + 1) * 128].reshape(32, 8, 128).astype(BF16)
            if last:
                send[:, 2 * pair + k, 0] = chunk
            else:
                send[:, 2 * pair + k] = chunk
    if last:
        send[:, :, 1] = acc[...].reshape(32, 4, 8, 128).astype(BF16)
        ones = jnp.ones((8, 128), F32)
        sums = lax.dot_general(
            ones,
            accb[...],
            (((1,), (1,)), ((), ())),
            preferred_element_type=F32,
            precision=lax.Precision.HIGHEST,
        )
        for k in range(4):
            bias_part[k : k + 1, :] = sums[:1, k * 128 : (k + 1) * 128]


VMEM = pl.BlockSpec(memory_space=pltpu.VMEM)
SMEM = pl.BlockSpec(memory_space=pltpu.SMEM)
HBM = pl.BlockSpec(memory_space=pltpu.HBM)


def shape(dims, kind):
    return jax.ShapeDtypeStruct(dims, kind)


def cost(flops, nbytes):
    return pl.CostEstimate(flops=flops, bytes_accessed=nbytes, transcendentals=0)


def whole(dims):
    return pl.BlockSpec(dims, lambda i: (0,) * len(dims))


VMEM_LIMIT = 20 * 1024 * 1024
BIG = 63_000_000
FIRST = 40_000_000


def call(body, ins, outs, scratch, in_specs, flops, nbytes, vmem=VMEM_LIMIT):
    many = isinstance(outs, (list, tuple))
    outs_list = list(outs) if many else [outs]
    out_specs = [whole(o.shape) for o in outs_list]
    return pl.pallas_call(
        body,
        grid=(1,),
        out_shape=outs_list if many else outs,
        in_specs=in_specs,
        out_specs=out_specs if many else out_specs[0],
        scratch_shapes=scratch,
        cost_estimate=cost(flops, nbytes),
        compiler_params=pltpu.CompilerParams(vmem_limit_bytes=vmem),
    )(*ins)


def exchange(array, axes):
    return lax.all_to_all(array, axes, split_axis=0, concat_axis=0, tiled=True)


def trig_base():
    phase = (np.arange(N)[:, None] * np.arange(LON)[None, :]) % LON
    angle = 2.0 * np.pi / LON * phase
    return jnp.asarray(np.concatenate([np.cos(angle), -np.sin(angle)], axis=1), BF16)


def program(checkpoints, final_cot, obs_cot, obs_time, wave_order, legendre, w_in, w_out, bias):
    states = checkpoints.reshape(STEPS, 512, N)
    final = final_cot.reshape(512, N)
    seen = obs_cot.reshape(4, FEAT * 8, 128)
    state_spec = pl.BlockSpec((1, 512, N), lambda i: (STEPS - 1, 0, 0))
    chunks = shape((DEV, 2, RHO, 128), BF16)
    tall = pltpu.VMEM((DEV * RHO, 128), F32)
    halves = pltpu.VMEM((2, 512, 128), F32)

    send, damped, table = call(
        first_kernel,
        (wave_order, legendre, final, states),
        (chunks, shape((RHO, 64, N), F32), shape((RHO, N, N), BF16)),
        [
            pltpu.VMEM((2, N, 128), F32),
            tall,
            tall,
            halves,
            halves,
        ],
        [SMEM, whole(legendre.shape), whole(final.shape), state_spec],
        300_000_000,
        4_000_000,
        BIG,
    )
    obs_shapes = [(1, 2, FEAT, 128)] * 4 + [(STEPS - 1, 2, FEAT, 128)] * 4
    obs_parts = pl.pallas_call(
        obs_kernel,
        grid=(2,),
        out_shape=[shape(d, BF16) for d in obs_shapes],
        in_specs=[SMEM, pl.BlockSpec((4, 512, 128), lambda g: (0, g, 0))],
        out_specs=[pl.BlockSpec(d[:2] + (64, 128), lambda g: (0, 0, g, 0)) for d in obs_shapes],
        cost_estimate=cost(10_000_000, 3_000_000),
        compiler_params=pltpu.CompilerParams(vmem_limit_bytes=BIG),
        name="obs",
    )(obs_time, seen)
    obs_cols = []
    for k, part in enumerate(obs_parts):
        if k % 4:
            part = lax.ppermute(part, "lev", [(i, (i + k) % 4) for i in range(4)])
        obs_cols.append(part)

    sums = ()
    for step in reversed(range(STEPS)):
        first = step == STEPS - 1
        last = step == 0
        got = exchange(send, ALL).reshape(32, 4, 2, RHO, 128)
        acc_shapes = [shape((2 * HID, 128), F32), shape((HID, 128), F32)]
        scratch = [
            pltpu.VMEM((2, 2, FEAT, 2 * N), BF16),
            pltpu.VMEM((2, 4, FEAT, 256), BF16),
            pltpu.VMEM((2, 2, FEAT, 256), BF16),
        ]
        outs = [shape((32, 4, RHO, 128), BF16)] + acc_shapes
        ins = [got, w_in, w_out]
        if first:
            ins += [wave_order.reshape(1, N), trig_base(), bias.reshape(1, HID)]
            outs += [shape((2 * N, LON), BF16), shape((HID, FEAT), BF16), shape((HID, 128), F32)]
            scratch += [pltpu.VMEM((4, 2, FEAT, 128), BF16)]
            ins += obs_cols[:4]
            specs = [whole(a.shape) for a in ins]
        else:
            ins += [trig, w_in_t, bias_wide, *sums]
            specs = [whole(a.shape) for a in ins]
            if step == STEPS - 2:
                ins += obs_cols[4:]
                specs = [whole(a.shape) for a in ins]
                outs.append(shape((STEPS - 1, 4, 2, FEAT, 128), BF16))
            else:
                ins.append(obs_all)
                specs.append(whole(obs_all.shape))
        if last:
            outs = [shape((32, 4, 2, RHO, 128), BF16), shape((4, 128), F32)]
            scratch = [pltpu.VMEM(a.shape, F32) for a in acc_shapes] + scratch
        back, *sums = call(
            functools.partial(column_kernel, first, last, step),
            ins,
            outs,
            scratch,
            specs,
            1_200_000_000,
            3_000_000,
            FIRST if first else VMEM_LIMIT,
        )
        if first:
            trig, w_in_t, bias_wide = sums[2:]
            sums = sums[:2]
        elif not last and len(sums) > 2:
            obs_all = sums.pop()
        if not last:
            back = exchange(back.reshape(DEV, RHO, 128), ALL)
            ins = [wave_order, back, damped, table, states]
            specs = [SMEM, whole(back.shape), whole(damped.shape), whole(table.shape), whole(states.shape)]
            outs = [chunks, shape((RHO, 64, N), F32)]
            scratch = [tall, tall, tall, halves]
            send, damped = call(
                functools.partial(turn_kernel, step - 1),
                ins,
                outs,
                scratch,
                specs,
                400_000_000,
                4_000_000,
            )
    back = exchange(back.reshape(DEV, 2, RHO, 128), ALL)
    (bias_part,) = sums
    parts = call(
        share_kernel,
        (back, bias_part),
        shape((DEV, 3, 4, 128), BF16),
        [],
        [whole(back.shape), whole(bias_part.shape)],
        1_000_000,
        1_000_000,
    )
    parts = exchange(parts, ALL)
    adjoint = call(
        last_kernel,
        (back, damped, table),
        shape((512, N), F32),
        [tall, halves],
        [whole(back.shape), whole(damped.shape), whole(table.shape)],
        100_000_000,
        3_000_000,
    )
    grad_w_in, grad_w_out, grad_bias = call(
        ending_kernel,
        (parts,),
        (shape((FEAT, HID), F32), shape((HID, FEAT), F32), shape((4, 128), F32)),
        [tall],
        [whole(parts.shape)],
        1_000_000,
        1_500_000,
    )
    return (adjoint.reshape(final_cot.shape), grad_w_in, grad_w_out, grad_bias.reshape(HID))


def solution(mesh):
    torus = Mesh(mesh.devices.reshape(4, 4, 2, mesh.shape["lev"]), ("band_0", "band_1", "band_2", "lev"))
    placed = (
        P(None, None, "lev", None, BAND, None),
        P(None, "lev", None, BAND, None),
        P(None, None, None, BAND, "lev"),
        P(),
        P(),
        P(BAND, None, None),
        P(),
        P(),
        P(),
    )
    return jax.shard_map(
        program,
        mesh=torus,
        in_specs=placed,
        out_specs=(P(None, "lev", None, BAND, None), P(), P(), P()),
        check_vma=False,
    )
```

```python
import functools

import jax
import jax.numpy as jnp
import numpy as np
from jax import lax
from jax.experimental import pallas as pl
from jax.experimental.pallas import tpu as pltpu
from jax.sharding import Mesh
from jax.sharding import PartitionSpec as P

BAND = ("band_0", "band_1", "band_2")
ALL = ("band_0", "band_1", "band_2", "lev")
F32 = jnp.float32
BF16 = jnp.bfloat16

RHO = 8
N = 256
LON = 512
FEAT = 128
HID = 512
STEPS = 4
VL = 32
DEV = 128


def mm(a, b):
    return jnp.dot(a, b, preferred_element_type=F32)


def mm_nt(a, b):
    return lax.dot_general(a, b, (((1,), (1,)), ((), ())), preferred_element_type=F32)


def lane_of(rows, lanes):
    return lax.broadcasted_iota(jnp.int32, (rows, lanes), 1)


def damping_row():
    n = lane_of(1, N).astype(F32)
    return 1.0 / (1.0 + 2.0 * n * (n + 1.0) / (N * N))


def halve(ref, halves):
    for h in range(2):
        halves[h] = ref[:, h * 128 : (h + 1) * 128]


def strided_rows(halves, rho):
    return jnp.concatenate(
        [
            jnp.concatenate(
                [halves[h, pl.ds(p * RHO + rho, VL, stride=2 * RHO), :] for h in range(2)], axis=1
            )
            for p in range(2)
        ],
        axis=0,
    )


def tangent_scale(m):
    return jnp.where(m == 0, 1.0 / LON, 0.5 / LON).astype(F32)


def synth_rho(table, tangent, state, rho, rows_t, rows_s):
    parts = []
    for s in (tangent, state):
        s = s.astype(BF16)
        parts += [s[:VL], s[:VL], s[VL:], s[VL:]]
    sums = mm_nt(table, jnp.concatenate(parts, axis=0))
    even = (lane_of(DEV, 2 * DEV) // VL) % 2 == 0
    both = jnp.where(even, sums[:DEV], sums[DEV:])
    rows_t[pl.ds(rho, DEV, stride=RHO), :] = both[:, :DEV]
    rows_s[pl.ds(rho, DEV, stride=RHO), :] = both[:, DEV:]


def write_chunks(send, rows_t, rows_s):
    send[:, 0] = rows_t[...].reshape(DEV, RHO, 128).astype(BF16)
    send[:, 1] = rows_s[...].reshape(DEV, RHO, 128).astype(BF16)


def first_kernel(
    waves, legendre, final, state, send, damped, table, tall, rows_t, rows_s, final_rows, state_rows
):
    damping = damping_row()
    band = lax.axis_index(BAND)
    halve(final, final_rows)
    halve(state.at[0], state_rows)
    degree = lane_of(N, N)
    for rho in range(RHO):
        m = waves[band * RHO + rho]
        kept = jnp.where(degree >= m, legendre[rho].astype(F32), 0.0)
        for h in range(2):
            tall[h] = kept[:, h * 128 : (h + 1) * 128]
        for jj in range(2):
            for h in range(2):
                part = tall[h, pl.ds(jj, DEV, stride=2), :].astype(BF16)
                table[rho, jj * DEV : (jj + 1) * DEV, h * 128 : (h + 1) * 128] = part
        now = damping * strided_rows(final_rows, rho)
        damped[rho] = now
        synth_rho(
            table[rho], now * tangent_scale(m), strided_rows(state_rows, rho), rho, rows_t, rows_s
        )
    write_chunks(send, rows_t, rows_s)


def adjoint_rho(rows, table, rho):
    back = rows[pl.ds(rho, DEV, stride=RHO), :].astype(BF16).T
    halves = []
    for p in range(2):
        at = 2 * p * VL
        halves.append(jnp.concatenate([back[at : at + VL], back[at + VL : at + 2 * VL]], axis=1))
    return mm(jnp.concatenate(halves, axis=0), table)


def turn_kernel(
    step, waves, back, damped_in, table, states, send, damped, rows, rows_t, rows_s, state_rows
):
    damping = damping_row()
    band = lax.axis_index(BAND)
    rows[...] = back[...].astype(F32).reshape(DEV * RHO, 128)
    halve(states.at[step], state_rows)
    for rho in range(RHO):
        damped[rho] = damping * (damped_in[rho] + adjoint_rho(rows, table[rho], rho))
    for rho in range(RHO):
        synth_rho(
            table[rho],
            damped[rho] * tangent_scale(waves[band * RHO + rho]),
            strided_rows(state_rows, rho),
            rho,
            rows_t,
            rows_s,
        )
    write_chunks(send, rows_t, rows_s)


def last_kernel(back, damped_in, table, out, rows, out_rows):
    rows[...] = back[:, 0].astype(F32).reshape(DEV * RHO, 128)
    for rho in range(RHO):
        now = damped_in[rho] + adjoint_rho(rows, table[rho], rho)
        for p in range(2):
            for h in range(2):
                part = now[p * VL : (p + 1) * VL, h * 128 : (h + 1) * 128]
                out_rows[h, pl.ds(p * RHO + rho, VL, stride=2 * RHO), :] = part
    for h in range(2):
        out[:, h * 128 : (h + 1) * 128] = out_rows[h]


def share_kernel(back, bias_part, send):
    total = jnp.sum(back[:, 1].astype(F32), axis=0)
    for part, rows in enumerate((total[:4], total[4:], bias_part[...])):
        send[:, part] = jnp.broadcast_to(rows[None], (DEV, 4, 128)).astype(BF16)


def ending_kernel(parts, w_in_out, w_out_out, bias_out, rows):
    for d in range(DEV):
        for half in range(2):
            rows[8 * d + 4 * half : 8 * d + 4 * half + 4, :] = parts[d, half].astype(F32)
    w_in_out[...] = rows[:HID].T
    w_out_out[...] = rows[HID:]
    bias_out[...] = jnp.sum(parts[:, 2].astype(F32), axis=0)


def fill_tables(waves, base, w_in, bias, trig, w_in_t, bias_wide):
    m = lax.broadcasted_iota(jnp.int32, (N, N), 0)
    weight = jnp.where(m == 0, 1.0, 2.0).astype(F32)
    pick = jnp.where(m == waves[...], weight, 0.0).T.astype(BF16)
    both = mm(pick, base[...]).astype(BF16)
    trig[:N] = both[:, :LON]
    trig[N:] = both[:, LON:]
    w_in_t[...] = w_in[...].astype(F32).T.astype(BF16)
    bias_wide[...] = jnp.broadcast_to(bias[...], (128, HID)).T


def obs_kernel(obs_time, obs, *outs):
    lev = lax.axis_index("lev")
    for k in range(4):
        to = lax.rem(lev + k, 4)
        for jj in range(2):
            pieces = [obs[i, pl.ds(2 * to + jj, 64, stride=8), :] for i in range(4)]
            for step in range(STEPS):
                total = jnp.zeros((64, 128), F32)
                for i in range(4):
                    total += jnp.where(obs_time[i] == step, 1.0, 0.0).astype(F32) * pieces[i]
                if step == STEPS - 1:
                    outs[k][0, jj] = total.astype(BF16)
                else:
                    outs[4 + k][step, jj] = total.astype(BF16)


def column_kernel(first, last, step, *refs):
    collect = step == STEPS - 2
    refs = list(refs)
    take = lambda count: [refs.pop(0) for _ in range(count)]
    got, w_in, w_out = take(3)
    if first:
        waves, base, bias_row = take(3)
        obs_parts = take(4)
        (send,) = take(1)
        acc, accb, trig, w_in_t, bias = take(5)
        turned, grid, grads, obs = refs
        lev = lax.axis_index("lev")
        for k in range(4):
            obs[lax.rem(lev + 4 - k, 4)] = obs_parts[k][0]
        fill_tables(waves, base, w_in, bias_row, trig, w_in_t, bias)
    else:
        trig, w_in_t, bias, acc_in, accb_in = take(5)
        if collect:
            obs_parts = take(4)
            send, acc, accb, obs_all, turned, grid, grads = refs
            lev = lax.axis_index("lev")
            for k in range(4):
                for s in range(STEPS - 1):
                    obs_all[s, lax.rem(lev + 4 - k, 4)] = obs_parts[k][s]
        else:
            obs_all, send = take(2)
            if last:
                (bias_part,) = take(1)
            acc, accb, turned, grid, grads = refs
        obs = obs_all.at[step]
    for kind in range(2):
        for y in range(4):
            x = got[:, y, kind].reshape(N, 128).T
            for p in range(2):
                for jj in range(2):
                    at = (2 * p + jj) * VL
                    turned[kind, jj, y * VL : (y + 1) * VL, p * N : (p + 1) * N] = x[at : at + VL]
    for kind in range(2):
        for jj in range(2):
            g = mm(turned[kind, jj], trig[...])
            g = jnp.concatenate(
                [g[(y * 4 + v) * 8 : (y * 4 + v + 1) * 8] for v in range(4) for y in range(4)], axis=0
            ).astype(BF16)
            for half in range(2):
                grid[kind, 2 * jj + half] = g[:, half * 256 : (half + 1) * 256]
    if first:
        acc[...] = jnp.zeros_like(acc)
        accb[...] = jnp.zeros_like(accb)
    else:
        acc[...] = acc_in[...]
        accb[...] = accb_in[...]

    def block(cb, carry):
        tangent = grid[0, cb]
        features = grid[1, cb]
        back = jnp.zeros((FEAT, 256), F32)
        for hb in range(1):
            rows = slice(hb * 512, (hb + 1) * 512)
            wide = bias[rows, :]
            pre = mm(w_in_t[rows, :], features) + jnp.concatenate([wide, wide], axis=1)
            logistic = 0.5 * jnp.tanh(0.5 * pre) + 0.5
            hidden = (pre * logistic).astype(BF16)
            pre_grad = mm(w_out[rows, :], tangent) * (logistic * (1.0 + pre * (1.0 - logistic)))
            low = pre_grad.astype(BF16)
            acc[rows, :] += mm_nt(low, features)
            acc[hb * 512 + HID : (hb + 1) * 512 + HID, :] += mm_nt(hidden, tangent)
            accb[rows, :] += pre_grad[:, :128] + pre_grad[:, 128:]
            back += mm(w_in[:, rows], low)
        jj = cb // 2
        half = cb % 2
        seen = jnp.concatenate([obs[2 * half + k, jj] for k in range(2)], axis=1)
        back += seen.astype(F32)
        back = jnp.concatenate(
            [back[(v * 4 + y) * 8 : (v * 4 + y + 1) * 8] for y in range(4) for v in range(4)], axis=0
        )
        grads[jj, half] = back.astype(BF16)
        return carry

    lax.fori_loop(0, 4, block, 0, unroll=True)

    real = (lane_of(N, 2 * 128) // 64) % 2 == 0
    for pair in range(2):
        rows = []
        for y in (2 * pair, 2 * pair + 1):
            for _ in range(2):
                for jj in range(2):
                    rows.append(
                        jnp.concatenate(
                            [grads[jj, half, y * VL : (y + 1) * VL, :] for half in range(2)], axis=1
                        )
                    )
        rows = jnp.concatenate(rows, axis=0)
        mixed = jnp.where(real, mm_nt(trig[:N], rows), mm_nt(trig[N:], rows))
        for k in range(2):
            chunk = mixed[:, k * 128 : (k + 1) * 128].reshape(32, 8, 128).astype(BF16)
            if last:
                send[:, 2 * pair + k, 0] = chunk
            else:
                send[:, 2 * pair + k] = chunk
    if last:
        send[:, :, 1] = acc[...].reshape(32, 4, 8, 128).astype(BF16)
        ones = jnp.ones((8, 128), F32)
        sums = lax.dot_general(
            ones,
            accb[...],
            (((1,), (1,)), ((), ())),
            preferred_element_type=F32,
            precision=lax.Precision.HIGHEST,
        )
        for k in range(4):
            bias_part[k : k + 1, :] = sums[:1, k * 128 : (k + 1) * 128]


VMEM = pl.BlockSpec(memory_space=pltpu.VMEM)
SMEM = pl.BlockSpec(memory_space=pltpu.SMEM)
HBM = pl.BlockSpec(memory_space=pltpu.HBM)


def shape(dims, kind):
    return jax.ShapeDtypeStruct(dims, kind)


def cost(flops, nbytes):
    return pl.CostEstimate(flops=flops, bytes_accessed=nbytes, transcendentals=0)


def whole(dims):
    return pl.BlockSpec(dims, lambda i: (0,) * len(dims))


VMEM_LIMIT = 20 * 1024 * 1024
BIG = 63_000_000
FIRST = 40_000_000


def call(body, ins, outs, scratch, in_specs, flops, nbytes, vmem=VMEM_LIMIT):
    many = isinstance(outs, (list, tuple))
    outs_list = list(outs) if many else [outs]
    out_specs = [whole(o.shape) for o in outs_list]
    return pl.pallas_call(
        body,
        grid=(1,),
        out_shape=outs_list if many else outs,
        in_specs=in_specs,
        out_specs=out_specs if many else out_specs[0],
        scratch_shapes=scratch,
        cost_estimate=cost(flops, nbytes),
        compiler_params=pltpu.CompilerParams(vmem_limit_bytes=vmem),
    )(*ins)


def exchange(array, axes):
    return lax.all_to_all(array, axes, split_axis=0, concat_axis=0, tiled=True)


def trig_base():
    phase = (np.arange(N)[:, None] * np.arange(LON)[None, :]) % LON
    angle = 2.0 * np.pi / LON * phase
    return jnp.asarray(np.concatenate([np.cos(angle), -np.sin(angle)], axis=1), BF16)


def program(checkpoints, final_cot, obs_cot, obs_time, wave_order, legendre, w_in, w_out, bias):
    states = checkpoints.reshape(STEPS, 512, N)
    final = final_cot.reshape(512, N)
    seen = obs_cot.reshape(4, FEAT * 8, 128)
    state_spec = pl.BlockSpec((1, 512, N), lambda i: (STEPS - 1, 0, 0))
    chunks = shape((DEV, 2, RHO, 128), BF16)
    tall = pltpu.VMEM((DEV * RHO, 128), F32)
    halves = pltpu.VMEM((2, 512, 128), F32)

    send, damped, table = call(
        first_kernel,
        (wave_order, legendre, final, states),
        (chunks, shape((RHO, 64, N), F32), shape((RHO, N, N), BF16)),
        [
            pltpu.VMEM((2, N, 128), F32),
            tall,
            tall,
            halves,
            halves,
        ],
        [SMEM, whole(legendre.shape), whole(final.shape), state_spec],
        300_000_000,
        4_000_000,
        BIG,
    )
    obs_shapes = [(1, 2, FEAT, 128)] * 4 + [(STEPS - 1, 2, FEAT, 128)] * 4
    obs_parts = pl.pallas_call(
        obs_kernel,
        grid=(2,),
        out_shape=[shape(d, BF16) for d in obs_shapes],
        in_specs=[SMEM, pl.BlockSpec((4, 512, 128), lambda g: (0, g, 0))],
        out_specs=[pl.BlockSpec(d[:2] + (64, 128), lambda g: (0, 0, g, 0)) for d in obs_shapes],
        cost_estimate=cost(10_000_000, 3_000_000),
        compiler_params=pltpu.CompilerParams(vmem_limit_bytes=BIG),
        name="obs",
    )(obs_time, seen)
    obs_cols = []
    for k, part in enumerate(obs_parts):
        if k % 4:
            part = lax.ppermute(part, "lev", [(i, (i + k) % 4) for i in range(4)])
        obs_cols.append(part)

    sums = ()
    for step in reversed(range(STEPS)):
        first = step == STEPS - 1
        last = step == 0
        got = exchange(send, ALL).reshape(32, 4, 2, RHO, 128)
        acc_shapes = [shape((2 * HID, 128), F32), shape((HID, 128), F32)]
        scratch = [
            pltpu.VMEM((2, 2, FEAT, 2 * N), BF16),
            pltpu.VMEM((2, 4, FEAT, 256), BF16),
            pltpu.VMEM((2, 2, FEAT, 256), BF16),
        ]
        outs = [shape((32, 4, RHO, 128), BF16)] + acc_shapes
        ins = [got, w_in, w_out]
        if first:
            ins += [wave_order.reshape(1, N), trig_base(), bias.reshape(1, HID)]
            outs += [shape((2 * N, LON), BF16), shape((HID, FEAT), BF16), shape((HID, 128), F32)]
            scratch += [pltpu.VMEM((4, 2, FEAT, 128), BF16)]
            ins += obs_cols[:4]
            specs = [whole(a.shape) for a in ins]
        else:
            ins += [trig, w_in_t, bias_wide, *sums]
            specs = [whole(a.shape) for a in ins]
            if step == STEPS - 2:
                ins += obs_cols[4:]
                specs = [whole(a.shape) for a in ins]
                outs.append(shape((STEPS - 1, 4, 2, FEAT, 128), BF16))
            else:
                ins.append(obs_all)
                specs.append(whole(obs_all.shape))
        if last:
            outs = [shape((32, 4, 2, RHO, 128), BF16), shape((4, 128), F32)]
            scratch = [pltpu.VMEM(a.shape, F32) for a in acc_shapes] + scratch
        back, *sums = call(
            functools.partial(column_kernel, first, last, step),
            ins,
            outs,
            scratch,
            specs,
            1_200_000_000,
            3_000_000,
            FIRST if first else VMEM_LIMIT,
        )
        if first:
            trig, w_in_t, bias_wide = sums[2:]
            sums = sums[:2]
        elif not last and len(sums) > 2:
            obs_all = sums.pop()
        if not last:
            back = exchange(back.reshape(DEV, RHO, 128), ALL)
            ins = [wave_order, back, damped, table, states]
            specs = [SMEM, whole(back.shape), whole(damped.shape), whole(table.shape), whole(states.shape)]
            outs = [chunks, shape((RHO, 64, N), F32)]
            scratch = [tall, tall, tall, halves]
            send, damped = call(
                functools.partial(turn_kernel, step - 1),
                ins,
                outs,
                scratch,
                specs,
                400_000_000,
                4_000_000,
            )
    back = exchange(back.reshape(DEV, 2, RHO, 128), ALL)
    (bias_part,) = sums
    parts = call(
        share_kernel,
        (back, bias_part),
        shape((DEV, 3, 4, 128), BF16),
        [],
        [whole(back.shape), whole(bias_part.shape)],
        1_000_000,
        1_000_000,
    )
    parts = exchange(parts, ALL)
    adjoint = call(
        last_kernel,
        (back, damped, table),
        shape((512, N), F32),
        [tall, halves],
        [whole(back.shape), whole(damped.shape), whole(table.shape)],
        100_000_000,
        3_000_000,
    )
    grad_w_in, grad_w_out, grad_bias = call(
        ending_kernel,
        (parts,),
        (shape((FEAT, HID), F32), shape((HID, FEAT), F32), shape((4, 128), F32)),
        [tall],
        [whole(parts.shape)],
        1_000_000,
        1_500_000,
    )
    return (adjoint.reshape(final_cot.shape), grad_w_in, grad_w_out, grad_bias.reshape(HID))


def solution(mesh):
    torus = Mesh(mesh.devices.reshape(4, 4, 2, mesh.shape["lev"]), ("band_0", "band_1", "band_2", "lev"))
    placed = (
        P(None, None, "lev", None, BAND, None),
        P(None, "lev", None, BAND, None),
        P(None, None, None, BAND, "lev"),
        P(),
        P(),
        P(BAND, None, None),
        P(),
        P(),
        P(),
    )
    return jax.shard_map(
        program,
        mesh=torus,
        in_specs=placed,
        out_specs=(P(None, "lev", None, BAND, None), P(), P(), P()),
        check_vma=False,
    )
```
